32 devices in a mesh: seq: 8 (over z, x), tp: 4 (over y, core).
Axes of the slice: x: 2, y: 2, z: 4, core: 2. Of those that a mesh axis runs over, the one named last changes fastest.
Arguments:
- tokens: bfloat16 [32768, 1024], P('seq'), may hold values from -16 to 16
- w_qkv: bfloat16 [3, 1024, 1024], P(None, None, 'tp'), as said below
- w_out: bfloat16 [1024, 1024], P('tp'), may hold values from -0.1875 to 0.1875
Outputs:
- mixed: bfloat16 [32768, 1024], P('seq', 'tp')
The draws below stay inside these ranges and needn't reach their ends.
Inputs may be any that keep to these rules, and one draw needn't show every extreme that they name: `w_qkv`: entries lie within six times 1024 ** -0.5 of zero.
All inputs are finite; a program needn't handle non-finite values.
Results may differ from the reference program's by a relative error of at most 0.03.
Values may be sent and summed in bfloat16 or wider, within the bound.
No kernel may reach another device: no remote copies, remote signals or barrier semaphores. Data moves between devices by JAX's collectives and lax.ppermute only.
A program may use at most 128 MiB of HBM per device.

```python
import jax
import jax.numpy as jnp
from jax import lax

D = 1024
HEADS = 16
HEAD_DIM = 64
LANDMARKS = 256
NEWTON = 6
TOK_DEV = 4096
TOKENS = 32768
N_SEQ = 8


def draw_tokens(key, part):
    first = jax.random.fold_in(key, 0)
    fifth = jax.random.fold_in(key, 4)
    base = jax.random.normal(first, (TOKENS, D), jnp.float32)
    offsets = jax.random.normal(fifth, (LANDMARKS, D), jnp.float32)
    seg_offsets = jnp.repeat(offsets, TOKENS // LANDMARKS, axis=0, total_repeat_length=TOKENS)
    base = base + seg_offsets
    return jnp.clip(base, -16.0, 16.0).astype(jnp.bfloat16)


def draw_w_qkv(key, part):
    limit = 6.0 * D ** (-0.5)
    weights = jax.random.normal(key, (3, D, D), jnp.float32) * D ** (-0.5)
    return jnp.clip(weights, -limit, limit).astype(jnp.bfloat16)


def block_levels(rng, extent, cuts, low, top_value):
    level = 1.0
    for dim, blocks in cuts:
        heights = jax.random.uniform(jax.random.fold_in(jax.random.fold_in(rng, 6), dim), (blocks,), jnp.float32, low / len(cuts), top_value / len(cuts))
        level = level * jnp.repeat(jnp.exp(heights), extent[dim] // blocks).reshape((-1,) + (1,) * (len(extent) - 1 - dim))
    return level


def normal_values(key, dims, width, most, cuts=(), kind=jnp.bfloat16):
    factor_of = block_levels(key, dims, cuts, -0.22, 0.18) if cuts else 1.0
    result = jax.random.normal(key, dims, jnp.float32) * width * factor_of
    return jnp.minimum(jnp.maximum(result, -most), most).astype(kind)


def setup_inputs(seed: int = 0) -> dict:
    keys = jax.random.split(jax.random.key(seed), 4)
    tokens = draw_tokens(jax.random.fold_in(keys[3], 71), 0)
    w_qkv = draw_w_qkv(jax.random.fold_in(keys[3], 71), 0)
    w_out = normal_values(keys[2], (D, D), D ** -0.5, 0.1875, ((0, 4),))
    return {"tokens": tokens, "w_qkv": w_qkv, "w_out": w_out}


def softmax_rows(logit_scores):
    top = jnp.max(logit_scores, axis=-1, keepdims=True)
    exponent_terms = jnp.exp(logit_scores - top)
    return exponent_terms / jnp.sum(exponent_terms, axis=-1, keepdims=True)


def newton_inverse(kernel_a):
    eye = jnp.eye(LANDMARKS, dtype=jnp.float32)
    hi = lax.Precision.HIGHEST
    colmax = jnp.max(jnp.sum(kernel_a, axis=0))
    rowmax = jnp.max(jnp.sum(kernel_a, axis=1))
    approx = kernel_a.T / (colmax * rowmax)
    for turn in range(NEWTON):
        prod_az = jnp.dot(kernel_a, approx, precision=hi)
        inner = jnp.dot(prod_az, 7.0 * eye - prod_az, precision=hi)
        outer = jnp.dot(prod_az, 15.0 * eye - inner, precision=hi)
        approx = 0.25 * jnp.dot(approx, 13.0 * eye - outer, precision=hi)
    return approx


def one_head(items):
    q_head, k_head, v_head, query_landmark_rows, key_landmark_rows = items
    score_scale = HEAD_DIM ** -0.5
    kernel_a = softmax_rows(jnp.dot(query_landmark_rows, key_landmark_rows.T, preferred_element_type=jnp.float32) * score_scale)
    pseudoinverse_kernel = newton_inverse(kernel_a)
    query_kernel_matrix = softmax_rows(jnp.dot(q_head, key_landmark_rows.T, preferred_element_type=jnp.float32) * score_scale).astype(jnp.bfloat16)
    logit_scores = (jnp.dot(query_landmark_rows, k_head.T, preferred_element_type=jnp.float32) * score_scale).reshape(LANDMARKS, N_SEQ, TOK_DEV)
    block_max = jnp.max(logit_scores, axis=2)
    exponent_terms = jnp.exp(logit_scores - block_max[:, :, None])
    block_total = jnp.sum(exponent_terms, axis=2)
    weights = exponent_terms.astype(jnp.bfloat16)
    block_acc = jnp.einsum("mnt,ntd->nmd", weights.astype(jnp.float32), v_head.reshape(N_SEQ, TOK_DEV, HEAD_DIM).astype(jnp.float32))
    row_max = jnp.max(block_max, axis=1)
    factor = jnp.exp(block_max - row_max[:, None])
    total = jnp.sum(block_total * factor, axis=1)
    landmark_value_rows = jnp.sum(block_acc * factor.T[:, :, None], axis=0) / total[:, None]
    center_kernel = jnp.dot(pseudoinverse_kernel, landmark_value_rows, precision=lax.Precision.HIGHEST).astype(jnp.bfloat16)
    return jnp.dot(query_kernel_matrix, center_kernel, preferred_element_type=jnp.float32).astype(jnp.bfloat16)


def reference(tokens, w_qkv, w_out):
    proj = lax.map(lambda weight: jnp.dot(tokens, weight, preferred_element_type=jnp.float32).astype(jnp.bfloat16), w_qkv)
    segment = TOKENS // LANDMARKS

    def marks(array):
        return jnp.mean(array.astype(jnp.float32).reshape(LANDMARKS, segment, D), axis=1).astype(jnp.bfloat16)

    q_marks = marks(proj[0])
    k_marks = marks(proj[1])

    def by_head(array, rows):
        return jnp.transpose(array.reshape(rows, HEADS, HEAD_DIM), (1, 0, 2))

    heads_out = lax.map(one_head, (by_head(proj[0], TOKENS), by_head(proj[1], TOKENS), by_head(proj[2], TOKENS), by_head(q_marks, LANDMARKS), by_head(k_marks, LANDMARKS)))
    attended = jnp.transpose(heads_out, (1, 0, 2)).reshape(TOKENS, D)
    return jnp.dot(attended, w_out, preferred_element_type=jnp.float32).astype(jnp.bfloat16)
```

```python
import functools
import math

import jax
import jax.numpy as jnp
from jax import lax
from jax.experimental import pallas as pl
from jax.experimental.pallas import tpu as pltpu
from jax.sharding import PartitionSpec as P

HEAD_DIM = 64
LANDMARKS = 256
NEWTON = 6
FACTOR = HEAD_DIM ** (-0.5) * math.log2(math.e)
PACK_ROWS = HEAD_DIM + 16
CHUNKS = 2


BF16 = jnp.bfloat16
F32 = jnp.float32


def cost(flops, nbytes, trans=0):
    return pl.CostEstimate(flops=flops, bytes_accessed=nbytes, transcendentals=trans)


def params(mib, axes=1):
    return pltpu.CompilerParams(
        dimension_semantics=("arbitrary",) * axes, vmem_limit_bytes=mib * 1024 * 1024
    )


def dot(a, b):
    return jnp.dot(a, b, preferred_element_type=F32)


def dot_nt(a, b):
    return lax.dot_general(a, b, (((1,), (1,)), ((), ())), preferred_element_type=F32)


def split2(x):
    hi = x.astype(BF16)
    lo = (x - hi.astype(F32)).astype(BF16)
    return hi, lo


def dot3(a, b):
    (ah, al), (bh, bl) = a, b
    return dot(jnp.concatenate([ah, ah, al], axis=1), jnp.concatenate([bh, bl, bh], axis=0))


def dot3_nt(a, b):
    (ah, al), (bh, bl) = a, b
    return dot_nt(jnp.concatenate([ah, ah, al], axis=1), jnp.concatenate([bh, bl, bh], axis=1))


def whole(shape):
    zeros = (0,) * len(shape)
    return pl.BlockSpec(shape, lambda *_: zeros)


def marks_kernel(segment, tok_ref, w_ref, out_ref, acc_ref):
    step = pl.program_id(0)
    tile = tok_ref.shape[0]
    count = acc_ref.shape[0]
    row = lax.broadcasted_iota(jnp.int32, (count, tile), 0)
    tok = lax.broadcasted_iota(jnp.int32, (count, tile), 1) + step * tile
    inside = (tok >= row * segment) & (tok < (row + 1) * segment)
    pick = jnp.where(inside, 1.0, 0.0).astype(BF16)
    part = dot(pick, tok_ref[...])

    @pl.when(step == 0)
    def _():
        acc_ref[...] = part

    @pl.when(step > 0)
    def _():
        acc_ref[...] += part

    @pl.when(step == pl.num_programs(0) - 1)
    def _():
        hi, lo = split2(acc_ref[...] * (1.0 / segment))
        width = w_ref.shape[2]
        for c in range(2):
            both = dot(hi, w_ref[c]) + dot(lo, w_ref[c])
            out_ref[:, c * width : (c + 1) * width] = (both * FACTOR).astype(BF16)


def local_marks(tokens, w_qkv, marks):
    n, d = tokens.shape
    width = w_qkv.shape[2]
    tile = min(1024, n)
    return pl.pallas_call(
        functools.partial(marks_kernel, n // marks),
        grid=(n // tile,),
        in_specs=[
            pl.BlockSpec((tile, d), lambda i: (i, 0)),
            pl.BlockSpec((2, d, width), lambda i: (0, 0, 0)),
        ],
        out_specs=whole((marks, 2 * width)),
        out_shape=jax.ShapeDtypeStruct((marks, 2 * width), BF16),
        scratch_shapes=[pltpu.VMEM((marks, d), F32)],
        compiler_params=params(12),
        cost_estimate=cost(2 * 256 * n * d, n * d * 2),
        name="marks",
    )(tokens, w_qkv)


def prep_kernel(far, wq_ref, wv_ref, wo_ref, send_ref, wvt_ref):
    d, width = send_ref.shape[0] - 2 * wo_ref.shape[0], send_ref.shape[1]
    owner = lax.axis_index("tp") ^ far
    send_ref[:d] = wq_ref[0]
    for j in range(2):
        at = pl.multiple_of((owner ^ j) * width, width)
        send_ref[d + j * width : d + (j + 1) * width] = wo_ref[:, pl.ds(at, width)]
    wvt_ref[...] = wv_ref[0].astype(F32).T.astype(BF16)


def prepare(w_qkv, w_out, far):
    _, d, width = w_qkv.shape
    send = (d + 2 * width, width)
    return pl.pallas_call(
        functools.partial(prep_kernel, far),
        grid=(1,),
        in_specs=[
            pl.BlockSpec((1, d, width), lambda i: (0, 0, 0)),
            pl.BlockSpec((1, d, width), lambda i: (2, 0, 0)),
            whole(w_out.shape),
        ],
        out_specs=[whole(send), whole((width, d))],
        out_shape=[jax.ShapeDtypeStruct(send, BF16), jax.ShapeDtypeStruct((width, d), BF16)],
        compiler_params=params(12),
        cost_estimate=cost(1_000_000_000, 4 << 20),
        name="prep",
    )(w_qkv, w_qkv, w_out)


def order_kernel(bit, x_ref, y_ref, out_ref, *k_refs):
    low = lax.rem(lax.div(lax.axis_index("seq"), bit), 2) == 0
    rows, cols = x_ref.shape
    refs = ((out_ref, 0),) + tuple((r, cols // 2) for r in k_refs)
    for first, a, b in ((low, x_ref, y_ref), (jnp.logical_not(low), y_ref, x_ref)):

        @pl.when(first)
        def _():
            for ref, at in refs:
                ref[:rows] = a[:, at:]
                ref[rows:] = b[:, at:]


def in_order(x, y, bit, split):
    rows, cols = x.shape
    shapes = [(2 * rows, cols)] + [(2 * rows, cols // 2)] * split
    return pl.pallas_call(
        functools.partial(order_kernel, bit),
        grid=(1,),
        in_specs=[whole(x.shape)] * 2,
        out_specs=[whole(s) for s in shapes],
        out_shape=[jax.ShapeDtypeStruct(s, BF16) for s in shapes],
        compiler_params=params(4),
        cost_estimate=cost(100_000_000, 4 * x.size),
        name="order",
    )(x, y)


def key_kernel(tok_ref, w_ref, out_ref):
    out_ref[...] = dot(tok_ref[...], w_ref[0]).astype(BF16)


def project_keys(tokens, w_qkv):
    n, d = tokens.shape
    width = w_qkv.shape[2]
    tile = min(512, n)
    return pl.pallas_call(
        key_kernel,
        grid=(n // tile,),
        in_specs=[
            pl.BlockSpec((tile, d), lambda i: (i, 0)),
            pl.BlockSpec((1, d, width), lambda i: (1, 0, 0)),
        ],
        out_specs=pl.BlockSpec((tile, width), lambda i: (i, 0)),
        out_shape=jax.ShapeDtypeStruct((n, width), BF16),
        compiler_params=params(8),
        cost_estimate=cost(2 * n * d * width, n * d * 2 + n * width * 2),
        name="keys",
    )(tokens, w_qkv)


def value_kernel(tok_ref, w_ref, out_ref):
    out_ref[...] = dot_nt(w_ref[...], tok_ref[...]).astype(BF16)


def project_values(tokens, w_value_t):
    n, d = tokens.shape
    width = w_value_t.shape[0]
    tile = min(512, n)
    return pl.pallas_call(
        value_kernel,
        grid=(n // tile,),
        in_specs=[pl.BlockSpec((tile, d), lambda i: (i, 0)), whole((width, d))],
        out_specs=pl.BlockSpec((width, tile), lambda i: (0, i)),
        out_shape=jax.ShapeDtypeStruct((width, n), BF16),
        compiler_params=params(8),
        cost_estimate=cost(2 * n * d * width, n * d * 2 + n * width * 2),
        name="values",
    )(tokens, w_value_t)


def pack(acc, top, total):
    def three(x):
        hi = x.astype(BF16).astype(F32)
        mid = (x - hi).astype(BF16).astype(F32)
        return hi, mid, x - hi - mid

    rows = three(top) + three(total)
    row = lax.broadcasted_iota(jnp.int32, (PACK_ROWS - HEAD_DIM, acc.shape[1]), 0)
    tail = jnp.zeros(row.shape, F32)
    for i, value in enumerate(rows):
        tail = jnp.where(row == i, value, tail)
    return jnp.concatenate([acc, tail], axis=0).astype(BF16)


def unpack(packed):
    x = packed.astype(F32)
    tail = x[HEAD_DIM:]
    top = tail[0:1] + tail[1:2] + tail[2:3]
    total = tail[3:4] + tail[4:5] + tail[5:6]
    return x[:HEAD_DIM], top, total


def merge(parts):
    parts = [unpack(p) for p in parts]
    top = functools.reduce(jnp.maximum, [p[1] for p in parts])
    factors = [jnp.exp2(p[1] - top) for p in parts]
    acc = sum(p[0] * f for p, f in zip(parts, factors))
    total = sum(p[2] * f for p, f in zip(parts, factors))
    return acc, top, total


def block_kernel(heads, chunk, k_ref, vt_ref, q_ref, mine_ref, theirs_ref, s_ref, qt_ref):
    step = pl.program_id(0)
    half = heads // 2
    parity = lax.rem(lax.axis_index("seq"), 2)
    first = jnp.where(step < half, (1 - parity) * half, parity * half)
    head = first + lax.rem(step, half)
    n, width = k_ref.shape

    @pl.when(step == 0)
    def _():
        qt_ref[...] = q_ref[...].astype(F32).T

    row = lax.broadcasted_iota(jnp.int32, qt_ref.shape, 0)
    inside = (row >= head * HEAD_DIM) & (row < (head + 1) * HEAD_DIM)
    qt = jnp.where(inside, qt_ref[...], 0.0).astype(BF16)
    top = None
    for c in range(n // chunk):
        s = dot(k_ref[c * chunk : (c + 1) * chunk], qt)
        s_ref[c * chunk : (c + 1) * chunk] = s
        m = jnp.max(s.reshape(chunk // 8, 8, s.shape[1]), axis=0)
        top = m if top is None else jnp.maximum(top, m)
    top = jnp.max(top, axis=0, keepdims=True)
    vt = vt_ref.at[pl.ds(pl.multiple_of(head * HEAD_DIM, HEAD_DIM), HEAD_DIM)]
    acc = None
    total = None
    for c in range(n // chunk):
        e = jnp.exp2(s_ref[c * chunk : (c + 1) * chunk] - top)
        t = jnp.sum(e.reshape(chunk // 8, 8, e.shape[1]), axis=0)
        a = dot(vt[:, c * chunk : (c + 1) * chunk], e.astype(BF16))
        acc = a if acc is None else acc + a
        total = t if total is None else total + t
    packed = pack(acc, top, jnp.sum(total, axis=0, keepdims=True))

    @pl.when(step < half)
    def _():
        theirs_ref[step] = packed

    @pl.when(step >= half)
    def _():
        mine_ref[step - half] = packed


def block_partials(keys, values_t, marks, heads):
    n, width = keys.shape
    half = heads // 2
    shape = (half, PACK_ROWS, LANDMARKS)
    return pl.pallas_call(
        functools.partial(block_kernel, heads, min(1024, n)),
        grid=(heads,),
        in_specs=[whole((n, width)), whole((width, n)), pl.BlockSpec((LANDMARKS, width), lambda i: (0, 0))],
        out_specs=[whole(shape), whole(shape)],
        out_shape=[jax.ShapeDtypeStruct(shape, BF16)] * 2,
        scratch_shapes=[pltpu.VMEM((n, LANDMARKS), F32), pltpu.VMEM((width, LANDMARKS), F32)],
        compiler_params=params(16),
        cost_estimate=cost(2 * heads * n * 256 * 256 * 3, n * width * 4, heads * n * LANDMARKS),
        name="block",
    )(keys, values_t, marks)


def merge_kernel(a_ref, b_ref, out_ref):
    for j in range(a_ref.shape[0]):
        out_ref[j] = pack(*merge([a_ref[j], b_ref[j]]))


def merge_pair(a, b):
    return pl.pallas_call(
        merge_kernel,
        in_specs=[whole(a.shape)] * 2,
        out_specs=whole(a.shape),
        grid=(1,),
        out_shape=jax.ShapeDtypeStruct(a.shape, BF16),
        compiler_params=params(4),
        cost_estimate=cost(200_000_000, 4 * a.size),
        name="merge",
    )(a, b)


def newton_kernel(heads, q_ref, k_ref, out_ref):
    half = heads // 2
    parity = lax.rem(lax.axis_index("seq"), 2)
    size = LANDMARKS
    lane = lax.broadcasted_iota(jnp.int32, q_ref.shape, 1)
    eye = jnp.where(
        lax.broadcasted_iota(jnp.int32, (size, size), 0)
        == lax.broadcasted_iota(jnp.int32, (size, size), 1),
        1.0,
        0.0,
    )
    kernels = []
    for j in range(half):
        head = parity * half + j
        inside = (lane >= head * HEAD_DIM) & (lane < (head + 1) * HEAD_DIM)
        q = jnp.where(inside, q_ref[...].astype(F32), 0.0).astype(BF16)
        scores = dot_nt(q, k_ref[...]) * (1.0 / FACTOR)
        e = jnp.exp2(scores - jnp.max(scores, axis=1, keepdims=True))
        a = e / jnp.sum(e, axis=1, keepdims=True)
        colmax = jnp.max(jnp.sum(a, axis=0, keepdims=True), axis=1, keepdims=True)
        rowmax = jnp.max(jnp.sum(a, axis=1, keepdims=True), axis=0, keepdims=True)
        out_ref[j] = a.T / (colmax * rowmax)
        kernels.append(split2(a))

    def turn(_, carry):
        prod = [dot3(kernels[j], split2(out_ref[j])) for j in range(half)]
        left = [split2(p) for p in prod]
        inner = [dot3(left[j], split2(7.0 * eye - prod[j])) for j in range(half)]
        outer = [dot3(left[j], split2(15.0 * eye - inner[j])) for j in range(half)]
        for j in range(half):
            out_ref[j] = 0.25 * dot3(split2(out_ref[j]), split2(13.0 * eye - outer[j]))
        return carry

    lax.fori_loop(0, NEWTON, turn, 0)


def pseudo_inverse(marks, heads):
    width = marks.shape[1] // 2
    half = heads // 2
    shape = (half, LANDMARKS, LANDMARKS)
    return pl.pallas_call(
        functools.partial(newton_kernel, heads),
        grid=(1,),
        in_specs=[
            pl.BlockSpec((LANDMARKS, width), lambda i: (0, 0)),
            pl.BlockSpec((LANDMARKS, width), lambda i: (0, 1)),
        ],
        out_specs=whole(shape),
        out_shape=jax.ShapeDtypeStruct(shape, F32),
        compiler_params=params(12),
        cost_estimate=cost(8_000_000_000, 1 << 20),
        name="newton",
    )(marks, marks)


def middle_kernel(count, *refs):
    parts, z_ref, out_ref = refs[:count], refs[count], refs[count + 1]
    for j in range(z_ref.shape[0]):
        acc, _, total = merge([p[j] for p in parts])
        out_ref[j] = dot3_nt(split2(acc / total), split2(z_ref[j])).astype(BF16)


def middle_rows(parts, pinv):
    half = pinv.shape[0]
    shape = (half, HEAD_DIM, LANDMARKS)
    return pl.pallas_call(
        functools.partial(middle_kernel, len(parts)),
        grid=(1,),
        in_specs=[whole(p.shape) for p in parts] + [whole(pinv.shape)],
        out_specs=whole(shape),
        out_shape=jax.ShapeDtypeStruct(shape, BF16),
        compiler_params=params(8),
        cost_estimate=cost(1_000_000_000, 1 << 20),
        name="middle",
    )(*parts, pinv)


def fill_keys(heads, ka_ref, kb_ref, kt_ref):
    for g, ref in enumerate((ka_ref, kb_ref)):
        kt = ref[...].astype(F32).T
        row = lax.broadcasted_iota(jnp.int32, kt.shape, 0)
        for h in range(heads):
            inside = (row >= h * HEAD_DIM) & (row < (h + 1) * HEAD_DIM)
            kt_ref[g * heads + h] = jnp.where(inside, kt, 0.0).astype(BF16)


def fill_middle(mine_ref, x_ref, y_ref, xy_ref, m_ref):
    parity = lax.rem(lax.axis_index("seq"), 2)
    half = mine_ref.shape[0]
    zeros = jnp.zeros((HEAD_DIM, LANDMARKS), F32)
    ones = jnp.ones((HEAD_DIM, LANDMARKS), F32)
    for group, (a, b) in enumerate(((mine_ref, x_ref), (y_ref, xy_ref))):
        for side in range(2):
            for j in range(half):
                mid = jnp.where(parity == side, a[j].astype(F32), b[j].astype(F32))
                blocks = [zeros, zeros, zeros, zeros]
                blocks[j % 2] = mid
                blocks[2 + j % 2] = ones
                full = jnp.concatenate(blocks, axis=0).T.astype(BF16)
                at = ((group * 2 + side) * half + j) * LANDMARKS
                m_ref[at : at + LANDMARKS] = full


def weigh(heads, tok_ref, wa_ref, wb_ref, kt_ref, p_ref):
    for g, w in enumerate((wa_ref[0], wb_ref[...])):
        q = dot(tok_ref[...], w).astype(BF16)
        for h in range(heads):
            s = dot(q, kt_ref[g * heads + h])
            e = jnp.exp2(s - jnp.max(s, axis=1, keepdims=True))
            at = (g * heads + h) * LANDMARKS
            p_ref[:, at : at + LANDMARKS] = e.astype(BF16)


def project(p_ref, m_ref, wo_ref, wb0_ref, wb1_ref, own_ref, send_ref):
    me = lax.axis_index("tp")
    pairs = m_ref.shape[0] // (2 * LANDMARKS)
    cols = []
    for g in range(pairs):
        rows = slice(g * 2 * LANDMARKS, (g + 1) * 2 * LANDMARKS)
        r = dot(p_ref[:, rows], m_ref[rows])
        cols.append((r[:, : 2 * HEAD_DIM] / r[:, 2 * HEAD_DIM :]).astype(BF16))
    per = pairs // 2
    first = jnp.concatenate(cols[:per], axis=1)
    second = jnp.concatenate(cols[per:], axis=1)
    width = own_ref.shape[1]
    for j, (out_ref, wb_ref) in enumerate(((own_ref, wb0_ref), (send_ref, wb1_ref))):
        at = pl.multiple_of((me ^ j) * width, width)
        mixed = dot(first, wo_ref[:, pl.ds(at, width)]) + dot(second, wb_ref[...])
        out_ref[...] = mixed.astype(BF16)


def final_kernel(heads, do_weigh, do_mix, *refs):
    refs = list(refs)
    step = pl.program_id(0)
    if do_weigh:
        tok_ref, wa_ref, wb_ref, ka_ref, kb_ref = refs[:5]
        del refs[:5]
    else:
        p_ref = refs.pop(0)
    if do_mix:
        mids, (wo_ref, wb0_ref, wb1_ref) = refs[:4], refs[4:7]
        own_ref, send_ref = refs[7:9]
        del refs[:9]
    else:
        p_ref = refs.pop(0)
    if do_weigh:
        kt_ref = refs.pop(0)
    if do_mix:
        m_ref = refs.pop(0)
    if do_weigh and do_mix:
        p_ref = refs.pop(0)

    @pl.when(step == 0)
    def _():
        if do_weigh:
            fill_keys(heads, ka_ref, kb_ref, kt_ref)
        if do_mix:
            fill_middle(*mids, m_ref)

    if do_weigh:
        weigh(heads, tok_ref, wa_ref, wb_ref, kt_ref, p_ref)
    if do_mix:
        project(p_ref, m_ref, wo_ref, wb0_ref, wb1_ref, own_ref, send_ref)


def final(start, count, heads, weigh_args=None, weights=None, mix_args=None):
    tile = min(512, count)
    steps = count // tile
    base = start // tile
    cols = 2 * heads * LANDMARKS
    args, in_specs, out_specs, out_shape, scratch = [], [], [], [], []
    flops = 0
    if weigh_args is not None:
        tokens, w_qkv, other, marks, k_other = weigh_args
        d, width = tokens.shape[1], w_qkv.shape[2]
        args += [tokens, w_qkv, other, marks, k_other]
        in_specs += [
            pl.BlockSpec((tile, d), lambda i: (base + i, 0)),
            pl.BlockSpec((1, d, width), lambda i: (0, 0, 0)),
            pl.BlockSpec((d, width), lambda i: (0, 0)),
            pl.BlockSpec((LANDMARKS, width), lambda i: (0, 1)),
            whole(k_other.shape),
        ]
        scratch += [pltpu.VMEM((2 * heads, width, LANDMARKS), BF16)]
        flops += 2 * count * 2 * (d * width + heads * 256 * 256)
    else:
        args += [weights]
        in_specs += [pl.BlockSpec((tile, cols), lambda i: (i, 0))]
    if mix_args is not None:
        mids, w_out, other = mix_args
        rows, total = w_out.shape
        width = other.shape[1]
        skip = (other.shape[0] - 2 * rows) // rows
        args += [*mids, w_out, other, other]
        in_specs += [whole(m.shape) for m in mids] + [whole((rows, total))]
        for j in range(2):
            in_specs += [pl.BlockSpec((rows, width), functools.partial(lambda j, i: (j, 0), skip + j))]
        out_specs += [pl.BlockSpec((tile, width), lambda i: (i, 0))] * 2
        out_shape += [jax.ShapeDtypeStruct((count, width), BF16)] * 2
        scratch += [pltpu.VMEM((cols, LANDMARKS), BF16)]
        flops += 2 * count * (cols * 256 + 4 * rows * width)
    else:
        out_specs += [pl.BlockSpec((tile, cols), lambda i: (i, 0))]
        out_shape += [jax.ShapeDtypeStruct((count, cols), BF16)]
    if weigh_args is not None and mix_args is not None:
        scratch += [pltpu.VMEM((tile, cols), BF16)]
    return pl.pallas_call(
        functools.partial(final_kernel, heads, weigh_args is not None, mix_args is not None),
        grid=(steps,),
        in_specs=in_specs,
        out_specs=out_specs,
        out_shape=out_shape,
        scratch_shapes=scratch,
        compiler_params=params(16),
        cost_estimate=cost(flops, count * 4096),
        name="final",
    )(*args)


def add_kernel(own_ref, got_ref, *refs):
    refs[-1][...] = (own_ref[...].astype(F32) + got_ref[...].astype(F32)).astype(BF16)


def add_into(out, own, got, chunk):
    count, width = own.shape
    tile = min(512, count)
    steps = count // tile
    row = pl.BlockSpec((tile, width), lambda i: (i, 0))
    old = [] if out is None else [out]
    return pl.pallas_call(
        add_kernel,
        grid=(steps,),
        in_specs=[row, row] + [pl.BlockSpec(memory_space=pl.ANY)] * len(old),
        out_specs=pl.BlockSpec((tile, width), lambda i: (chunk * steps + i, 0)),
        out_shape=jax.ShapeDtypeStruct((CHUNKS * count, width), BF16),
        input_output_aliases={2: 0} if old else {},
        compiler_params=params(4),
        cost_estimate=cost(500_000_000, 6 * own.size),
        name="add",
    )(own, got, *old)


def swap(x, axes, sizes, steps):
    pairs = []
    total = math.prod(sizes)
    for i in range(total):
        rest, at = i, []
        for size in reversed(sizes):
            at.append(rest % size)
            rest //= size
        at = [a ^ s for a, s in zip(reversed(at), steps)]
        to = 0
        for a, size in zip(at, sizes):
            to = to * size + a
        pairs.append((i, to))
    return lax.ppermute(x, axes if len(axes) > 1 else axes[0], pairs)


def gather_doubling(x, n_seq):
    bit = 1
    while bit < n_seq:
        y = swap(x, ("seq",), (n_seq,), (bit,))
        x, *keys = in_order(x, y, bit, 2 * bit == n_seq)
        bit *= 2
    return x, keys[0]


def on_device(n_seq, n_tp, tokens, w_qkv, w_out):
    width = w_out.shape[0]
    heads = width // HEAD_DIM
    far = n_tp // 2

    local = local_marks(tokens, w_qkv, LANDMARKS // n_seq)
    send, w_value_t = prepare(w_qkv, w_out, far)
    other = swap(send, ("tp",), (n_tp,), (far,))
    marks, k_marks = gather_doubling(local, n_seq)
    keys = project_keys(tokens, w_qkv)
    values_t = project_values(tokens, w_value_t)
    k_other = swap(k_marks, ("tp",), (n_tp,), (far,))

    mine, theirs = block_partials(keys, values_t, marks, heads)
    pair = merge_pair(mine, swap(theirs, ("seq",), (n_seq,), (1,)))
    parts = [pair] + [swap(pair, ("seq",), (n_seq,), (2 * j,)) for j in range(1, n_seq // 2)]
    pinv = pseudo_inverse(marks, heads)
    mid = middle_rows(parts, pinv)
    sizes = (n_seq, n_tp)
    mids = [mid] + [swap(mid, ("seq", "tp"), sizes, s) for s in ((1, 0), (0, far), (1, far))]
    weigh_args = (tokens, w_qkv, other, marks, k_other)
    mix_args = (mids, w_out, other)
    count = tokens.shape[0] // CHUNKS
    (weights,) = final(0, count, heads, weigh_args=weigh_args)
    out = None
    for c in range(CHUNKS):
        if c == 0:
            own, send = final(0, count, heads, weights=weights, mix_args=mix_args)
        else:
            own, send = final(c * count, count, heads, weigh_args=weigh_args, mix_args=mix_args)
        out = add_into(out, own, swap(send, ("tp",), (n_tp,), (1,)), c)
    return out


def solution(mesh):
    n_seq, n_tp = mesh.shape["seq"], mesh.shape["tp"]
    if n_tp != 4 or n_seq < 2 or n_seq & (n_seq - 1):
        raise ValueError("unsupported mesh")
    in_specs = (P("seq", None), P(None, None, "tp"), P("tp", None))
    return jax.shard_map(
        functools.partial(on_device, n_seq, n_tp),
        mesh=mesh,
        in_specs=in_specs,
        out_specs=P("seq", "tp"),
        check_vma=False,
    )
```

```python
import functools
import math

import jax
import jax.numpy as jnp
from jax import lax
from jax.experimental import pallas as pl
from jax.experimental.pallas import tpu as pltpu
from jax.sharding import PartitionSpec as P

HEAD_DIM = 64
LANDMARKS = 256
NEWTON = 6
FACTOR = HEAD_DIM ** (-0.5) * math.log2(math.e)
PACK_ROWS = HEAD_DIM + 16
CHUNKS = 2


BF16 = jnp.bfloat16
F32 = jnp.float32


def cost(flops, nbytes, trans=0):
    return pl.CostEstimate(flops=flops, bytes_accessed=nbytes, transcendentals=trans)


def params(mib, axes=1):
    return pltpu.CompilerParams(
        dimension_semantics=("arbitrary",) * axes, vmem_limit_bytes=mib * 1024 * 1024
    )


def dot(a, b):
    return jnp.dot(a, b, preferred_element_type=F32)


def dot_nt(a, b):
    return lax.dot_general(a, b, (((1,), (1,)), ((), ())), preferred_element_type=F32)


def split2(x):
    hi = x.astype(BF16)
    lo = (x - hi.astype(F32)).astype(BF16)
    return hi, lo


def dot3(a, b):
    (ah, al), (bh, bl) = a, b
    return dot(jnp.concatenate([ah, ah, al], axis=1), jnp.concatenate([bh, bl, bh], axis=0))


def dot3_nt(a, b):
    (ah, al), (bh, bl) = a, b
    return dot_nt(jnp.concatenate([ah, ah, al], axis=1), jnp.concatenate([bh, bl, bh], axis=1))


def whole(shape):
    zeros = (0,) * len(shape)
    return pl.BlockSpec(shape, lambda *_: zeros)


def means_kernel(segment, count, tok_hbm, out_ref, tok_ref, sems):
    n = tok_ref.shape[0]
    tile = n // count
    copies = []
    for c in range(count):
        rows = pl.ds(c * tile, tile)
        copies.append(pltpu.make_async_copy(tok_hbm.at[rows], tok_ref.at[rows], sems.at[c]))
    for copy in copies:
        copy.start()
    marks = out_ref.shape[0]
    row = lax.broadcasted_iota(jnp.int32, (marks, tile), 0)
    tok = lax.broadcasted_iota(jnp.int32, (marks, tile), 1)
    acc = None
    for c, copy in enumerate(copies):
        at = tok + c * tile
        inside = (at >= row * segment) & (at < (row + 1) * segment)
        pick = jnp.where(inside, 1.0, 0.0).astype(BF16)
        copy.wait()
        part = dot(pick, tok_ref[c * tile : (c + 1) * tile])
        acc = part if acc is None else acc + part
    out_ref[...] = acc * (1.0 / segment)


def token_means(tokens, marks):
    n, d = tokens.shape
    count = 8
    return pl.pallas_call(
        functools.partial(means_kernel, n // marks, count),
        grid=(1,),
        in_specs=[pl.BlockSpec(memory_space=pltpu.HBM)],
        out_specs=[whole((marks, d)), whole((n, d))],
        out_shape=[jax.ShapeDtypeStruct((marks, d), F32), jax.ShapeDtypeStruct((n, d), BF16)],
        scratch_shapes=[pltpu.SemaphoreType.DMA((count,))],
        compiler_params=params(40),
        cost_estimate=cost(6_000_000_000, n * d * 2),
        name="means",
    )(tokens)


def marks_kernel(mean_ref, w_ref, out_ref):
    hi, lo = split2(mean_ref[...])
    width = w_ref.shape[2]
    for c in range(2):
        both = dot(hi, w_ref[c]) + dot(lo, w_ref[c])
        out_ref[:, c * width : (c + 1) * width] = (both * FACTOR).astype(BF16)


def local_marks(means, w_qkv):
    marks, d = means.shape
    width = w_qkv.shape[2]
    return pl.pallas_call(
        marks_kernel,
        grid=(1,),
        in_specs=[whole((marks, d)), pl.BlockSpec((2, d, width), lambda i: (0, 0, 0))],
        out_specs=whole((marks, 2 * width)),
        out_shape=jax.ShapeDtypeStruct((marks, 2 * width), BF16),
        compiler_params=params(6),
        cost_estimate=cost(500_000_000, 1 << 20),
        name="marks",
    )(means, w_qkv)


def prep_kernel(far, wq_ref, wv_ref, wo_ref, send_ref, wvt_ref):
    d, width = send_ref.shape[0] - 2 * wo_ref.shape[0], send_ref.shape[1]
    owner = lax.axis_index("tp") ^ far
    send_ref[:d] = wq_ref[0]
    for j in range(2):
        at = pl.multiple_of((owner ^ j) * width, width)
        send_ref[d + j * width : d + (j + 1) * width] = wo_ref[:, pl.ds(at, width)]
    wvt_ref[...] = wv_ref[0].astype(F32).T.astype(BF16)


def prepare(w_qkv, w_out, far):
    _, d, width = w_qkv.shape
    send = (d + 2 * width, width)
    return pl.pallas_call(
        functools.partial(prep_kernel, far),
        grid=(1,),
        in_specs=[
            pl.BlockSpec((1, d, width), lambda i: (0, 0, 0)),
            pl.BlockSpec((1, d, width), lambda i: (2, 0, 0)),
            whole(w_out.shape),
        ],
        out_specs=[whole(send), whole((width, d))],
        out_shape=[jax.ShapeDtypeStruct(send, BF16), jax.ShapeDtypeStruct((width, d), BF16)],
        compiler_params=params(12),
        cost_estimate=cost(1_000_000_000, 4 << 20),
        name="prep",
    )(w_qkv, w_qkv, w_out)


def order_kernel(bit, x_ref, y_ref, out_ref, *k_refs):
    low = lax.rem(lax.div(lax.axis_index("seq"), bit), 2) == 0
    rows, cols = x_ref.shape
    refs = ((out_ref, 0),) + tuple((r, cols // 2) for r in k_refs)
    for first, a, b in ((low, x_ref, y_ref), (jnp.logical_not(low), y_ref, x_ref)):

        @pl.when(first)
        def _():
            for ref, at in refs:
                ref[:rows] = a[:, at:]
                ref[rows:] = b[:, at:]


def in_order(x, y, bit, split):
    rows, cols = x.shape
    shapes = [(2 * rows, cols)] + [(2 * rows, cols // 2)] * split
    return pl.pallas_call(
        functools.partial(order_kernel, bit),
        grid=(1,),
        in_specs=[whole(x.shape)] * 2,
        out_specs=[whole(s) for s in shapes],
        out_shape=[jax.ShapeDtypeStruct(s, BF16) for s in shapes],
        compiler_params=params(4),
        cost_estimate=cost(100_000_000, 4 * x.size),
        name="order",
    )(x, y)


def rows_kernel(tok_ref, w_ref, out_ref):
    out_ref[...] = dot(tok_ref[...], w_ref[0]).astype(BF16)


def project_rows(tokens, w_qkv, which):
    n, d = tokens.shape
    width = w_qkv.shape[2]
    tile = min(1024, n)
    return pl.pallas_call(
        rows_kernel,
        grid=(n // tile,),
        in_specs=[
            pl.BlockSpec((tile, d), lambda i: (i, 0)),
            pl.BlockSpec((1, d, width), lambda i: (which, 0, 0)),
        ],
        out_specs=pl.BlockSpec((tile, width), lambda i: (i, 0)),
        out_shape=jax.ShapeDtypeStruct((n, width), BF16),
        compiler_params=params(10),
        cost_estimate=cost(2 * n * d * width, n * d * 2 + n * width * 2),
        name="rows",
    )(tokens, w_qkv)


def value_kernel(tok_ref, w_ref, out_ref):
    out_ref[...] = dot_nt(w_ref[...], tok_ref[...]).astype(BF16)


def project_values(tokens, w_value_t):
    n, d = tokens.shape
    width = w_value_t.shape[0]
    tile = min(1024, n)
    return pl.pallas_call(
        value_kernel,
        grid=(n // tile,),
        in_specs=[pl.BlockSpec((tile, d), lambda i: (i, 0)), whole((width, d))],
        out_specs=pl.BlockSpec((width, tile), lambda i: (0, i)),
        out_shape=jax.ShapeDtypeStruct((width, n), BF16),
        compiler_params=params(10),
        cost_estimate=cost(2 * n * d * width, n * d * 2 + n * width * 2),
        name="values",
    )(tokens, w_value_t)


def pack(acc, top, total):
    def three(x):
        hi = x.astype(BF16).astype(F32)
        mid = (x - hi).astype(BF16).astype(F32)
        return hi, mid, x - hi - mid

    rows = three(top) + three(total)
    row = lax.broadcasted_iota(jnp.int32, (PACK_ROWS - HEAD_DIM, acc.shape[1]), 0)
    tail = jnp.zeros(row.shape, F32)
    for i, value in enumerate(rows):
        tail = jnp.where(row == i, value, tail)
    return jnp.concatenate([acc, tail], axis=0).astype(BF16)


def unpack(packed):
    x = packed.astype(F32)
    tail = x[HEAD_DIM:]
    top = tail[0:1] + tail[1:2] + tail[2:3]
    total = tail[3:4] + tail[4:5] + tail[5:6]
    return x[:HEAD_DIM], top, total


def merge(parts):
    parts = [unpack(p) for p in parts]
    top = functools.reduce(jnp.maximum, [p[1] for p in parts])
    factors = [jnp.exp2(p[1] - top) for p in parts]
    acc = sum(p[0] * f for p, f in zip(parts, factors))
    total = sum(p[2] * f for p, f in zip(parts, factors))
    return acc, top, total


def block_kernel(heads, chunk, k_ref, vt_ref, q_ref, mine_ref, theirs_ref, s_ref):
    half = heads // 2
    parity = lax.rem(lax.axis_index("seq"), 2)
    n = k_ref.shape[0]
    queries = q_ref[...].astype(F32).T
    row = lax.broadcasted_iota(jnp.int32, queries.shape, 0)
    order = [(1 - parity) * half + j for j in range(half)] + [parity * half + j for j in range(half)]
    last = None
    for stage in range(heads + 1):
        top = acc = total = None
        if stage < heads:
            low = order[stage] * HEAD_DIM
            inside = (row >= low) & (row < low + HEAD_DIM)
            qt = jnp.where(inside, queries, 0.0).astype(BF16)
        if stage > 0:
            at = pl.multiple_of(order[stage - 1] * HEAD_DIM, HEAD_DIM)
            vt = vt_ref.at[pl.ds(at, HEAD_DIM)]
        for c in range(n // chunk):
            rows = slice(c * chunk, (c + 1) * chunk)
            if stage < heads:
                s = dot(k_ref[rows], qt)
                s_ref[stage % 2, rows] = s
                m = jnp.max(s.reshape(chunk // 8, 8, s.shape[1]), axis=0)
                top = m if top is None else jnp.maximum(top, m)
            if stage > 0:
                e = jnp.exp2(s_ref[(stage - 1) % 2, rows] - last)
                t = jnp.sum(e.reshape(chunk // 8, 8, e.shape[1]), axis=0)
                a = dot(vt[:, rows], e.astype(BF16))
                acc = a if acc is None else acc + a
                total = t if total is None else total + t
        if stage > 0:
            packed = pack(acc, last, jnp.sum(total, axis=0, keepdims=True))
            if stage <= half:
                theirs_ref[stage - 1] = packed
            else:
                mine_ref[stage - 1 - half] = packed
        if stage < heads:
            last = jnp.max(top, axis=0, keepdims=True)


def block_partials(keys, values_t, marks, heads):
    n, width = keys.shape
    half = heads // 2
    shape = (half, PACK_ROWS, LANDMARKS)
    return pl.pallas_call(
        functools.partial(block_kernel, heads, min(512, n)),
        grid=(1,),
        in_specs=[whole((n, width)), whole((width, n)), pl.BlockSpec((LANDMARKS, width), lambda i: (0, 0))],
        out_specs=[whole(shape), whole(shape)],
        out_shape=[jax.ShapeDtypeStruct(shape, BF16)] * 2,
        scratch_shapes=[pltpu.VMEM((2, n, LANDMARKS), F32)],
        compiler_params=params(24),
        cost_estimate=cost(2 * heads * n * 256 * 256 * 3, n * width * 4, heads * n * LANDMARKS),
        name="block",
    )(keys, values_t, marks)


def merge_kernel(a_ref, b_ref, out_ref):
    for j in range(a_ref.shape[0]):
        out_ref[j] = pack(*merge([a_ref[j], b_ref[j]]))


def merge_pair(a, b):
    return pl.pallas_call(
        merge_kernel,
        in_specs=[whole(a.shape)] * 2,
        out_specs=whole(a.shape),
        grid=(1,),
        out_shape=jax.ShapeDtypeStruct(a.shape, BF16),
        compiler_params=params(4),
        cost_estimate=cost(200_000_000, 4 * a.size),
        name="merge",
    )(a, b)


def newton_kernel(heads, q_ref, k_ref, out_ref, x_ref):
    half = heads // 2
    parity = lax.rem(lax.axis_index("seq"), 2)
    size = LANDMARKS
    lane = lax.broadcasted_iota(jnp.int32, q_ref.shape, 1)
    eye = jnp.where(
        lax.broadcasted_iota(jnp.int32, (size, size), 0)
        == lax.broadcasted_iota(jnp.int32, (size, size), 1),
        1.0,
        0.0,
    )
    for j in range(half):
        head = parity * half + j
        inside = (lane >= head * HEAD_DIM) & (lane < (head + 1) * HEAD_DIM)
        q = jnp.where(inside, q_ref[...].astype(F32), 0.0).astype(BF16)
        scores = dot_nt(q, k_ref[...]) * (1.0 / FACTOR)
        e = jnp.exp2(scores - jnp.max(scores, axis=1, keepdims=True))
        a = e / jnp.sum(e, axis=1, keepdims=True)
        colmax = jnp.max(jnp.sum(a, axis=0, keepdims=True), axis=1, keepdims=True)
        rowmax = jnp.max(jnp.sum(a, axis=1, keepdims=True), axis=0, keepdims=True)
        z = a.T / (colmax * rowmax)
        out_ref[j] = z
        x_ref[j] = dot3(split2(a), split2(z))

    def factor(j):
        x = x_ref[j]
        left = split2(x)
        square = dot3(left, left)
        return left, split2(13.0 * eye - 15.0 * x + dot3(split2(square), split2(7.0 * eye - x)))

    def turn(_, carry):
        for left, right, j in [factor(j) + (j,) for j in range(half)]:
            x_ref[j] = 0.25 * dot3(left, right)
            out_ref[j] = 0.25 * dot3(split2(out_ref[j]), right)
        return carry

    lax.fori_loop(0, NEWTON - 1, turn, 0)
    for j in range(half):
        out_ref[j] = 0.25 * dot3(split2(out_ref[j]), factor(j)[1])


def pseudo_inverse(marks, heads):
    width = marks.shape[1] // 2
    half = heads // 2
    shape = (half, LANDMARKS, LANDMARKS)
    return pl.pallas_call(
        functools.partial(newton_kernel, heads),
        grid=(1,),
        in_specs=[
            pl.BlockSpec((LANDMARKS, width), lambda i: (0, 0)),
            pl.BlockSpec((LANDMARKS, width), lambda i: (0, 1)),
        ],
        out_specs=whole(shape),
        out_shape=jax.ShapeDtypeStruct(shape, F32),
        scratch_shapes=[pltpu.VMEM(shape, F32)],
        compiler_params=params(12),
        cost_estimate=cost(8_000_000_000, 1 << 20),
        name="newton",
    )(marks, marks)


def middle_kernel(count, *refs):
    parts, z_ref, out_ref = refs[:count], refs[count], refs[count + 1]
    for j in range(z_ref.shape[0]):
        acc, _, total = merge([p[j] for p in parts])
        out_ref[j] = dot3_nt(split2(acc / total), split2(z_ref[j])).astype(BF16)


def middle_rows(parts, pinv):
    half = pinv.shape[0]
    shape = (half, HEAD_DIM, LANDMARKS)
    return pl.pallas_call(
        functools.partial(middle_kernel, len(parts)),
        grid=(1,),
        in_specs=[whole(p.shape) for p in parts] + [whole(pinv.shape)],
        out_specs=whole(shape),
        out_shape=jax.ShapeDtypeStruct(shape, BF16),
        compiler_params=params(8),
        cost_estimate=cost(1_000_000_000, 1 << 20),
        name="middle",
    )(*parts, pinv)


def fill_keys(heads, ka_ref, kb_ref, kt_ref):
    for g, ref in enumerate((ka_ref, kb_ref)):
        kt = ref[...].astype(F32).T
        row = lax.broadcasted_iota(jnp.int32, kt.shape, 0)
        for h in range(heads):
            inside = (row >= h * HEAD_DIM) & (row < (h + 1) * HEAD_DIM)
            kt_ref[g * heads + h] = jnp.where(inside, kt, 0.0).astype(BF16)


def fill_middle(mine_ref, x_ref, y_ref, xy_ref, m_ref):
    parity = lax.rem(lax.axis_index("seq"), 2)
    half = mine_ref.shape[0]
    zeros = jnp.zeros((HEAD_DIM, LANDMARKS), F32)
    ones = jnp.ones((HEAD_DIM, LANDMARKS), F32)
    for group, (a, b) in enumerate(((mine_ref, x_ref), (y_ref, xy_ref))):
        for side in range(2):
            for j in range(half):
                mid = jnp.where(parity == side, a[j].astype(F32), b[j].astype(F32))
                blocks = [zeros, zeros, zeros, zeros]
                blocks[j % 2] = mid
                blocks[2 + j % 2] = ones
                full = jnp.concatenate(blocks, axis=0).T.astype(BF16)
                at = ((group * 2 + side) * half + j) * LANDMARKS
                m_ref[at : at + LANDMARKS] = full


def weigh(heads, tok_ref, q_ref, wb_ref, kt_ref, p_ref):
    for g in range(2):
        q = q_ref[...] if g == 0 else dot(tok_ref[...], wb_ref[...]).astype(BF16)
        for h in range(heads):
            s = dot(q, kt_ref[g * heads + h])
            e = jnp.exp2(s - jnp.max(s, axis=1, keepdims=True))
            at = (g * heads + h) * LANDMARKS
            p_ref[:, at : at + LANDMARKS] = e.astype(BF16)


def project(p_ref, m_ref, wo_ref, wb0_ref, wb1_ref, own_ref, send_ref):
    me = lax.axis_index("tp")
    pairs = m_ref.shape[0] // (2 * LANDMARKS)
    cols = []
    for g in range(pairs):
        rows = slice(g * 2 * LANDMARKS, (g + 1) * 2 * LANDMARKS)
        r = dot(p_ref[:, rows], m_ref[rows])
        cols.append((r[:, : 2 * HEAD_DIM] / r[:, 2 * HEAD_DIM :]).astype(BF16))
    per = pairs // 2
    first = jnp.concatenate(cols[:per], axis=1)
    second = jnp.concatenate(cols[per:], axis=1)
    width = own_ref.shape[1]
    for j, (out_ref, wb_ref) in enumerate(((own_ref, wb0_ref), (send_ref, wb1_ref))):
        at = pl.multiple_of((me ^ j) * width, width)
        mixed = dot(first, wo_ref[:, pl.ds(at, width)]) + dot(second, wb_ref[...])
        out_ref[...] = mixed.astype(BF16)


def final_kernel(heads, do_weigh, do_mix, *refs):
    refs = list(refs)
    step = pl.program_id(0)
    if do_weigh:
        tok_ref, q_ref, wb_ref, ka_ref, kb_ref = refs[:5]
        del refs[:5]
    else:
        p_ref = refs.pop(0)
    if do_mix:
        mids, (wo_ref, wb0_ref, wb1_ref) = refs[:4], refs[4:7]
        own_ref, send_ref = refs[7:9]
        del refs[:9]
    else:
        p_ref = refs.pop(0)
    if do_weigh:
        kt_ref = refs.pop(0)
    if do_mix:
        m_ref = refs.pop(0)
    if do_weigh and do_mix:
        p_ref = refs.pop(0)

    @pl.when(step == 0)
    def _():
        if do_weigh:
            fill_keys(heads, ka_ref, kb_ref, kt_ref)
        if do_mix:
            fill_middle(*mids, m_ref)

    if do_weigh:
        weigh(heads, tok_ref, q_ref, wb_ref, kt_ref, p_ref)
    if do_mix:
        project(p_ref, m_ref, wo_ref, wb0_ref, wb1_ref, own_ref, send_ref)


def final(start, count, heads, weigh_args=None, weights=None, mix_args=None):
    tile = min(1024, count)
    steps = count // tile
    base = start // tile
    cols = 2 * heads * LANDMARKS
    args, in_specs, out_specs, out_shape, scratch = [], [], [], [], []
    flops = 0
    if weigh_args is not None:
        tokens, queries, other, marks, k_other = weigh_args
        d, width = tokens.shape[1], queries.shape[1]
        args += [tokens, queries, other, marks, k_other]
        in_specs += [
            pl.BlockSpec((tile, d), lambda i: (base + i, 0)),
            pl.BlockSpec((tile, width), lambda i: (base + i, 0)),
            pl.BlockSpec((d, width), lambda i: (0, 0)),
            pl.BlockSpec((LANDMARKS, width), lambda i: (0, 1)),
            whole(k_other.shape),
        ]
        scratch += [pltpu.VMEM((2 * heads, width, LANDMARKS), BF16)]
        flops += 2 * count * (d * width + 2 * heads * 256 * 256)
    else:
        args += [weights]
        in_specs += [pl.BlockSpec((tile, cols), lambda i: (i, 0))]
    if mix_args is not None:
        mids, w_out, other = mix_args
        rows, total = w_out.shape
        width = other.shape[1]
        skip = (other.shape[0] - 2 * rows) // rows
        args += [*mids, w_out, other, other]
        in_specs += [whole(m.shape) for m in mids] + [whole((rows, total))]
        for j in range(2):
            in_specs += [pl.BlockSpec((rows, width), functools.partial(lambda j, i: (j, 0), skip + j))]
        out_specs += [pl.BlockSpec((tile, width), lambda i: (i, 0))] * 2
        out_shape += [jax.ShapeDtypeStruct((count, width), BF16)] * 2
        scratch += [pltpu.VMEM((cols, LANDMARKS), BF16)]
        flops += 2 * count * (cols * 256 + 4 * rows * width)
    else:
        out_specs += [pl.BlockSpec((tile, cols), lambda i: (i, 0))]
        out_shape += [jax.ShapeDtypeStruct((count, cols), BF16)]
    if weigh_args is not None and mix_args is not None:
        scratch += [pltpu.VMEM((tile, cols), BF16)]
    return pl.pallas_call(
        functools.partial(final_kernel, heads, weigh_args is not None, mix_args is not None),
        grid=(steps,),
        in_specs=in_specs,
        out_specs=out_specs,
        out_shape=out_shape,
        scratch_shapes=scratch,
        compiler_params=params(24),
        cost_estimate=cost(flops, count * 4096),
        name="final",
    )(*args)


def add_kernel(own_ref, got_ref, *refs):
    refs[-1][...] = (own_ref[...].astype(F32) + got_ref[...].astype(F32)).astype(BF16)


def add_into(out, own, got, chunk):
    count, width = own.shape
    tile = min(1024, count)
    steps = count // tile
    row = pl.BlockSpec((tile, width), lambda i: (i, 0))
    old = [] if out is None else [out]
    return pl.pallas_call(
        add_kernel,
        grid=(steps,),
        in_specs=[row, row] + [pl.BlockSpec(memory_space=pl.ANY)] * len(old),
        out_specs=pl.BlockSpec((tile, width), lambda i: (chunk * steps + i, 0)),
        out_shape=jax.ShapeDtypeStruct((CHUNKS * count, width), BF16),
        input_output_aliases={2: 0} if old else {},
        compiler_params=params(4),
        cost_estimate=cost(500_000_000, 6 * own.size),
        name="add",
    )(own, got, *old)


def swap(x, axes, sizes, steps):
    pairs = []
    total = math.prod(sizes)
    for i in range(total):
        rest, at = i, []
        for size in reversed(sizes):
            at.append(rest % size)
            rest //= size
        at = [a ^ s for a, s in zip(reversed(at), steps)]
        to = 0
        for a, size in zip(at, sizes):
            to = to * size + a
        pairs.append((i, to))
    return lax.ppermute(x, axes if len(axes) > 1 else axes[0], pairs)


def gather_doubling(x, n_seq):
    bit = 1
    while bit < n_seq:
        y = swap(x, ("seq",), (n_seq,), (bit,))
        x, *keys = in_order(x, y, bit, 2 * bit == n_seq)
        bit *= 2
    return x, keys[0]


def on_device(n_seq, n_tp, tokens, w_qkv, w_out):
    width = w_out.shape[0]
    heads = width // HEAD_DIM
    far = n_tp // 2

    means, tokens = token_means(tokens, LANDMARKS // n_seq)
    local = local_marks(means, w_qkv)
    send, w_value_t = prepare(w_qkv, w_out, far)
    other = swap(send, ("tp",), (n_tp,), (far,))
    marks, k_marks = gather_doubling(local, n_seq)
    keys = project_rows(tokens, w_qkv, 1)
    queries = project_rows(tokens, w_qkv, 0)
    values_t = project_values(tokens, w_value_t)
    k_other = swap(k_marks, ("tp",), (n_tp,), (far,))

    mine, theirs = block_partials(keys, values_t, marks, heads)
    pair = merge_pair(mine, swap(theirs, ("seq",), (n_seq,), (1,)))
    parts = [pair] + [swap(pair, ("seq",), (n_seq,), (2 * j,)) for j in range(1, n_seq // 2)]
    pinv = pseudo_inverse(marks, heads)
    mid = middle_rows(parts, pinv)
    sizes = (n_seq, n_tp)
    mids = [mid] + [swap(mid, ("seq", "tp"), sizes, s) for s in ((1, 0), (0, far), (1, far))]
    weigh_args = (tokens, queries, other, marks, k_other)
    mix_args = (mids, w_out, other)
    count = tokens.shape[0] // CHUNKS
    (weights,) = final(0, count, heads, weigh_args=weigh_args)
    out = None
    for c in range(CHUNKS):
        if c == 0:
            own, send = final(0, count, heads, weights=weights, mix_args=mix_args)
        else:
            own, send = final(c * count, count, heads, weigh_args=weigh_args, mix_args=mix_args)
        out = add_into(out, own, swap(send, ("tp",), (n_tp,), (1,)), c)
    return out


def solution(mesh):
    n_seq, n_tp = mesh.shape["seq"], mesh.shape["tp"]
    if n_tp != 4 or n_seq < 2 or n_seq & (n_seq - 1):
        raise ValueError("unsupported mesh")
    in_specs = (P("seq", None), P(None, None, "tp"), P("tp", None))
    return jax.shard_map(
        functools.partial(on_device, n_seq, n_tp),
        mesh=mesh,
        in_specs=in_specs,
        out_specs=P("seq", "tp"),
        check_vma=False,
    )
```

```python
import functools
import math

import jax
import jax.numpy as jnp
from jax import lax
from jax.experimental import pallas as pl
from jax.experimental.pallas import tpu as pltpu
from jax.sharding import PartitionSpec as P

HEAD_DIM = 64
LANDMARKS = 256
NEWTON = 6
FACTOR = HEAD_DIM ** (-0.5) * math.log2(math.e)
PACK_ROWS = HEAD_DIM + 16
TILES = 8


BF16 = jnp.bfloat16
F32 = jnp.float32


def cost(flops, nbytes, trans=0):
    return pl.CostEstimate(flops=flops, bytes_accessed=nbytes, transcendentals=trans)


def params(mib, axes=1):
    return pltpu.CompilerParams(
        dimension_semantics=("arbitrary",) * axes, vmem_limit_bytes=mib * 1024 * 1024
    )


def dot(a, b):
    return jnp.dot(a, b, preferred_element_type=F32)


def dot_nt(a, b):
    return lax.dot_general(a, b, (((1,), (1,)), ((), ())), preferred_element_type=F32)


def split2(x):
    hi = x.astype(BF16)
    lo = (x - hi.astype(F32)).astype(BF16)
    return hi, lo


def dot3(a, b):
    (ah, al), (bh, bl) = a, b
    return dot(jnp.concatenate([ah, ah, al], axis=1), jnp.concatenate([bh, bl, bh], axis=0))


def dot3_nt(a, b):
    (ah, al), (bh, bl) = a, b
    return dot_nt(jnp.concatenate([ah, ah, al], axis=1), jnp.concatenate([bh, bl, bh], axis=1))


def whole(shape):
    zeros = (0,) * len(shape)
    return pl.BlockSpec(shape, lambda *_: zeros)


def means_kernel(segment, count, tok_hbm, out_ref, tok_ref, sems):
    n = tok_ref.shape[0]
    tile = n // count
    copies = []
    for c in range(count):
        rows = pl.ds(c * tile, tile)
        copies.append(pltpu.make_async_copy(tok_hbm.at[rows], tok_ref.at[rows], sems.at[c]))
    for copy in copies:
        copy.start()
    marks = out_ref.shape[0]
    row = lax.broadcasted_iota(jnp.int32, (marks, tile), 0)
    tok = lax.broadcasted_iota(jnp.int32, (marks, tile), 1)
    acc = None
    for c, copy in enumerate(copies):
        at = tok + c * tile
        inside = (at >= row * segment) & (at < (row + 1) * segment)
        pick = jnp.where(inside, 1.0, 0.0).astype(BF16)
        copy.wait()
        part = dot(pick, tok_ref[c * tile : (c + 1) * tile])
        acc = part if acc is None else acc + part
    out_ref[...] = acc * (1.0 / segment)


def token_means(tokens, marks):
    n, d = tokens.shape
    count = 16
    return pl.pallas_call(
        functools.partial(means_kernel, n // marks, count),
        grid=(1,),
        in_specs=[pl.BlockSpec(memory_space=pltpu.HBM)],
        out_specs=[whole((marks, d)), whole((n, d))],
        out_shape=[jax.ShapeDtypeStruct((marks, d), F32), jax.ShapeDtypeStruct((n, d), BF16)],
        scratch_shapes=[pltpu.SemaphoreType.DMA((count,))],
        compiler_params=params(40),
        cost_estimate=cost(6_000_000_000, n * d * 2),
        name="means",
    )(tokens)


def marks_kernel(mean_ref, w_ref, out_ref):
    hi, lo = split2(mean_ref[...])
    width = w_ref.shape[2]
    for c in range(2):
        both = dot(hi, w_ref[c]) + dot(lo, w_ref[c])
        out_ref[:, c * width : (c + 1) * width] = (both * FACTOR).astype(BF16)


def local_marks(means, w_qkv):
    marks, d = means.shape
    width = w_qkv.shape[2]
    return pl.pallas_call(
        marks_kernel,
        grid=(1,),
        in_specs=[whole((marks, d)), pl.BlockSpec((2, d, width), lambda i: (0, 0, 0))],
        out_specs=whole((marks, 2 * width)),
        out_shape=jax.ShapeDtypeStruct((marks, 2 * width), BF16),
        compiler_params=params(6),
        cost_estimate=cost(500_000_000, 1 << 20),
        name="marks",
    )(means, w_qkv)


def prep_kernel(far, wq_ref, wv_ref, wo_ref, send_ref, wvt_ref):
    d, width = send_ref.shape[0] - 2 * wo_ref.shape[0], send_ref.shape[1]
    owner = lax.axis_index("tp") ^ far
    send_ref[:d] = wq_ref[0]
    for j in range(2):
        at = pl.multiple_of((owner ^ j) * width, width)
        send_ref[d + j * width : d + (j + 1) * width] = wo_ref[:, pl.ds(at, width)]
    wvt_ref[...] = wv_ref[0].astype(F32).T.astype(BF16)


def prepare(w_qkv, w_out, far):
    _, d, width = w_qkv.shape
    send = (d + 2 * width, width)
    return pl.pallas_call(
        functools.partial(prep_kernel, far),
        grid=(1,),
        in_specs=[
            pl.BlockSpec((1, d, width), lambda i: (0, 0, 0)),
            pl.BlockSpec((1, d, width), lambda i: (2, 0, 0)),
            whole(w_out.shape),
        ],
        out_specs=[whole(send), whole((width, d))],
        out_shape=[jax.ShapeDtypeStruct(send, BF16), jax.ShapeDtypeStruct((width, d), BF16)],
        compiler_params=params(12),
        cost_estimate=cost(1_000_000_000, 4 << 20),
        name="prep",
    )(w_qkv, w_qkv, w_out)


def order_kernel(bit, x_ref, y_ref, out_ref, *k_refs):
    low = lax.rem(lax.div(lax.axis_index("seq"), bit), 2) == 0
    rows, cols = x_ref.shape
    refs = ((out_ref, 0),) + tuple((r, cols // 2) for r in k_refs)
    for first, a, b in ((low, x_ref, y_ref), (jnp.logical_not(low), y_ref, x_ref)):

        @pl.when(first)
        def _():
            for ref, at in refs:
                ref[:rows] = a[:, at:]
                ref[rows:] = b[:, at:]


def in_order(x, y, bit, split):
    rows, cols = x.shape
    shapes = [(2 * rows, cols)] + [(2 * rows, cols // 2)] * split
    return pl.pallas_call(
        functools.partial(order_kernel, bit),
        grid=(1,),
        in_specs=[whole(x.shape)] * 2,
        out_specs=[whole(s) for s in shapes],
        out_shape=[jax.ShapeDtypeStruct(s, BF16) for s in shapes],
        compiler_params=params(4),
        cost_estimate=cost(100_000_000, 4 * x.size),
        name="order",
    )(x, y)


def rows_kernel(tok_ref, w_ref, out_ref):
    out_ref[...] = dot(tok_ref[...], w_ref[0]).astype(BF16)


def project_rows(tokens, w_qkv, which):
    n, d = tokens.shape
    width = w_qkv.shape[2]
    tile = min(2048, n)
    return pl.pallas_call(
        rows_kernel,
        grid=(n // tile,),
        in_specs=[
            pl.BlockSpec((tile, d), lambda i: (i, 0)),
            pl.BlockSpec((1, d, width), lambda i: (which, 0, 0)),
        ],
        out_specs=pl.BlockSpec((tile, width), lambda i: (i, 0)),
        out_shape=jax.ShapeDtypeStruct((n, width), BF16),
        compiler_params=params(12),
        cost_estimate=cost(2 * n * d * width, n * d * 2 + n * width * 2),
        name="rows",
    )(tokens, w_qkv)


def value_kernel(tok_ref, w_ref, out_ref):
    out_ref[...] = dot_nt(w_ref[...], tok_ref[...]).astype(BF16)


def project_values(tokens, w_value_t):
    n, d = tokens.shape
    width = w_value_t.shape[0]
    tile = min(2048, n)
    return pl.pallas_call(
        value_kernel,
        grid=(n // tile,),
        in_specs=[pl.BlockSpec((tile, d), lambda i: (i, 0)), whole((width, d))],
        out_specs=pl.BlockSpec((width, tile), lambda i: (0, i)),
        out_shape=jax.ShapeDtypeStruct((width, n), BF16),
        compiler_params=params(12),
        cost_estimate=cost(2 * n * d * width, n * d * 2 + n * width * 2),
        name="values",
    )(tokens, w_value_t)


def pack(acc, top, total):
    def three(x):
        hi = x.astype(BF16).astype(F32)
        mid = (x - hi).astype(BF16).astype(F32)
        return hi, mid, x - hi - mid

    rows = three(top) + three(total)
    row = lax.broadcasted_iota(jnp.int32, (PACK_ROWS - HEAD_DIM, acc.shape[1]), 0)
    tail = jnp.zeros(row.shape, F32)
    for i, value in enumerate(rows):
        tail = jnp.where(row == i, value, tail)
    return jnp.concatenate([acc, tail], axis=0).astype(BF16)


def unpack(packed):
    x = packed.astype(F32)
    tail = x[HEAD_DIM:]
    top = tail[0:1] + tail[1:2] + tail[2:3]
    total = tail[3:4] + tail[4:5] + tail[5:6]
    return x[:HEAD_DIM], top, total


def merge(parts):
    parts = [unpack(p) for p in parts]
    top = functools.reduce(jnp.maximum, [p[1] for p in parts])
    factors = [jnp.exp2(p[1] - top) for p in parts]
    acc = sum(p[0] * f for p, f in zip(parts, factors))
    total = sum(p[2] * f for p, f in zip(parts, factors))
    return acc, top, total


def block_kernel(heads, chunk, k_ref, vt_ref, q_ref, mine_ref, theirs_ref, s_ref):
    half = heads // 2
    parity = lax.rem(lax.axis_index("seq"), 2)
    n = k_ref.shape[0]
    queries = q_ref[...].astype(F32).T
    row = lax.broadcasted_iota(jnp.int32, queries.shape, 0)
    order = [(1 - parity) * half + j for j in range(half)] + [parity * half + j for j in range(half)]
    last = None
    for stage in range(heads + 1):
        top = acc = total = None
        if stage < heads:
            low = order[stage] * HEAD_DIM
            inside = (row >= low) & (row < low + HEAD_DIM)
            qt = jnp.where(inside, queries, 0.0).astype(BF16)
        if stage > 0:
            at = pl.multiple_of(order[stage - 1] * HEAD_DIM, HEAD_DIM)
            vt = vt_ref.at[pl.ds(at, HEAD_DIM)]
        for c in range(n // chunk):
            rows = slice(c * chunk, (c + 1) * chunk)
            if stage < heads:
                s = dot(k_ref[rows], qt)
                s_ref[stage % 2, rows] = s
                m = jnp.max(s.reshape(chunk // 8, 8, s.shape[1]), axis=0)
                top = m if top is None else jnp.maximum(top, m)
            if stage > 0:
                e = jnp.exp2(s_ref[(stage - 1) % 2, rows] - last)
                t = jnp.sum(e.reshape(chunk // 8, 8, e.shape[1]), axis=0)
                a = dot(vt[:, rows], e.astype(BF16))
                acc = a if acc is None else acc + a
                total = t if total is None else total + t
        if stage > 0:
            packed = pack(acc, last, jnp.sum(total, axis=0, keepdims=True))
            if stage <= half:
                theirs_ref[stage - 1] = packed
            else:
                mine_ref[stage - 1 - half] = packed
        if stage < heads:
            last = jnp.max(top, axis=0, keepdims=True)


def block_partials(keys, values_t, marks, heads):
    n, width = keys.shape
    half = heads // 2
    shape = (half, PACK_ROWS, LANDMARKS)
    return pl.pallas_call(
        functools.partial(block_kernel, heads, min(1024, n)),
        grid=(1,),
        in_specs=[whole((n, width)), whole((width, n)), pl.BlockSpec((LANDMARKS, width), lambda i: (0, 0))],
        out_specs=[whole(shape), whole(shape)],
        out_shape=[jax.ShapeDtypeStruct(shape, BF16)] * 2,
        scratch_shapes=[pltpu.VMEM((2, n, LANDMARKS), F32)],
        compiler_params=params(24),
        cost_estimate=cost(2 * heads * n * 256 * 256 * 3, n * width * 4, heads * n * LANDMARKS),
        name="block",
    )(keys, values_t, marks)


def merge_kernel(a_ref, b_ref, out_ref):
    for j in range(a_ref.shape[0]):
        out_ref[j] = pack(*merge([a_ref[j], b_ref[j]]))


def merge_pair(a, b):
    return pl.pallas_call(
        merge_kernel,
        in_specs=[whole(a.shape)] * 2,
        out_specs=whole(a.shape),
        grid=(1,),
        out_shape=jax.ShapeDtypeStruct(a.shape, BF16),
        compiler_params=params(4),
        cost_estimate=cost(200_000_000, 4 * a.size),
        name="merge",
    )(a, b)


def newton_kernel(heads, tile, marks_q, marks_k, k_other, tok_ref, q_ref, wb_ref, out_ref, p_ref, x_ref, kt_ref):
    half = heads // 2
    parity = lax.rem(lax.axis_index("seq"), 2)
    size = LANDMARKS
    lane = lax.broadcasted_iota(jnp.int32, marks_q.shape, 1)
    eye = jnp.where(
        lax.broadcasted_iota(jnp.int32, (size, size), 0)
        == lax.broadcasted_iota(jnp.int32, (size, size), 1),
        1.0,
        0.0,
    )
    fill_keys(heads, marks_k, k_other, kt_ref)
    for j in range(half):
        head = parity * half + j
        inside = (lane >= head * HEAD_DIM) & (lane < (head + 1) * HEAD_DIM)
        q = jnp.where(inside, marks_q[...].astype(F32), 0.0).astype(BF16)
        scores = dot_nt(q, marks_k[...]) * (1.0 / FACTOR)
        e = jnp.exp2(scores - jnp.max(scores, axis=1, keepdims=True))
        a = e / jnp.sum(e, axis=1, keepdims=True)
        colmax = jnp.max(jnp.sum(a, axis=0, keepdims=True), axis=1, keepdims=True)
        rowmax = jnp.max(jnp.sum(a, axis=1, keepdims=True), axis=0, keepdims=True)
        z = a.T / (colmax * rowmax)
        out_ref[j] = z
        x_ref[j] = dot3(split2(a), split2(z))

    def weights_of(rows, query, group, h):
        s = dot(query, kt_ref[group * heads + h])
        e = jnp.exp2(s - jnp.max(s, axis=1, keepdims=True))
        at = (group * heads + h) * LANDMARKS
        p_ref[rows, at : at + LANDMARKS] = e.astype(BF16)

    def turn(i, more):
        rows = pl.ds(pl.multiple_of(i * tile, tile), tile)
        half_heads = range(heads // 2), range(heads // 2, heads)
        xs = [x_ref[j] for j in range(half)]
        left = [split2(x) for x in xs]
        square = [dot3(p, p) for p in left]
        other = dot(tok_ref[rows], wb_ref[...]).astype(BF16)
        own = q_ref[rows]
        for h in half_heads[0]:
            weights_of(rows, own, 0, h)
        q = [dot3(split2(square[j]), split2(7.0 * eye - xs[j])) for j in range(half)]
        for h in half_heads[1]:
            weights_of(rows, own, 0, h)
        right = [split2(13.0 * eye - 15.0 * xs[j] + q[j]) for j in range(half)]
        for j in range(half):
            if more:
                x_ref[j] = 0.25 * dot3(left[j], right[j])
            out_ref[j] = 0.25 * dot3(split2(out_ref[j]), right[j])
        for h in range(heads):
            weights_of(rows, other, 1, h)

    def body(i, carry):
        turn(i, True)
        return carry

    lax.fori_loop(0, NEWTON - 1, body, 0)
    turn(NEWTON - 1, False)


def pseudo_inverse(marks, heads, k_other, tokens, queries, other):
    width = marks.shape[1] // 2
    half = heads // 2
    shape = (half, LANDMARKS, LANDMARKS)
    n, d = tokens.shape
    tile = n // TILES
    weights = (NEWTON * tile, 2 * heads * LANDMARKS)
    return pl.pallas_call(
        functools.partial(newton_kernel, heads, tile),
        grid=(1,),
        in_specs=[
            pl.BlockSpec((LANDMARKS, width), lambda i: (0, 0)),
            pl.BlockSpec((LANDMARKS, width), lambda i: (0, 1)),
            whole(k_other.shape),
            whole(tokens.shape),
            whole(queries.shape),
            pl.BlockSpec((d, width), lambda i: (0, 0)),
        ],
        out_specs=[whole(shape), whole(weights)],
        out_shape=[jax.ShapeDtypeStruct(shape, F32), jax.ShapeDtypeStruct(weights, BF16)],
        scratch_shapes=[
            pltpu.VMEM(shape, F32),
            pltpu.VMEM((2 * heads, width, LANDMARKS), BF16),
        ],
        compiler_params=params(16),
        cost_estimate=cost(16_000_000_000, 1 << 20),
        name="newton",
    )(marks, marks, k_other, tokens, queries, other)


def middle_kernel(count, *refs):
    parts, z_ref, out_ref = refs[:count], refs[count], refs[count + 1]
    for j in range(z_ref.shape[0]):
        acc, _, total = merge([p[j] for p in parts])
        out_ref[j] = dot3_nt(split2(acc / total), split2(z_ref[j])).astype(BF16)


def middle_rows(parts, pinv):
    half = pinv.shape[0]
    shape = (half, HEAD_DIM, LANDMARKS)
    return pl.pallas_call(
        functools.partial(middle_kernel, len(parts)),
        grid=(1,),
        in_specs=[whole(p.shape) for p in parts] + [whole(pinv.shape)],
        out_specs=whole(shape),
        out_shape=jax.ShapeDtypeStruct(shape, BF16),
        compiler_params=params(8),
        cost_estimate=cost(1_000_000_000, 1 << 20),
        name="middle",
    )(*parts, pinv)


def fill_keys(heads, ka_ref, kb_ref, kt_ref):
    for g, ref in enumerate((ka_ref, kb_ref)):
        kt = ref[...].astype(F32).T
        row = lax.broadcasted_iota(jnp.int32, kt.shape, 0)
        for h in range(heads):
            inside = (row >= h * HEAD_DIM) & (row < (h + 1) * HEAD_DIM)
            kt_ref[g * heads + h] = jnp.where(inside, kt, 0.0).astype(BF16)


def fill_middle(mine_ref, x_ref, y_ref, xy_ref, m_ref):
    parity = lax.rem(lax.axis_index("seq"), 2)
    half = mine_ref.shape[0]
    zeros = jnp.zeros((HEAD_DIM, LANDMARKS), F32)
    ones = jnp.ones((HEAD_DIM, LANDMARKS), F32)
    for group, (a, b) in enumerate(((mine_ref, x_ref), (y_ref, xy_ref))):
        for side in range(2):
            for j in range(half):
                mid = jnp.where(parity == side, a[j].astype(F32), b[j].astype(F32))
                blocks = [zeros, zeros, zeros, zeros]
                blocks[j % 2] = mid
                blocks[2 + j % 2] = ones
                full = jnp.concatenate(blocks, axis=0).T.astype(BF16)
                at = ((group * 2 + side) * half + j) * LANDMARKS
                m_ref[at : at + LANDMARKS] = full


def weigh(heads, tok_ref, q_ref, wb_ref, kt_ref, p_ref):
    for g in range(2):
        q = q_ref[...] if g == 0 else dot(tok_ref[...], wb_ref[...]).astype(BF16)
        for h in range(heads):
            s = dot(q, kt_ref[g * heads + h])
            e = jnp.exp2(s - jnp.max(s, axis=1, keepdims=True))
            at = (g * heads + h) * LANDMARKS
            p_ref[:, at : at + LANDMARKS] = e.astype(BF16)


def project(p_ref, m_ref, wo_ref, wb0_ref, wb1_ref, own_ref, send_ref):
    me = lax.axis_index("tp")
    pairs = m_ref.shape[0] // (2 * LANDMARKS)
    cols = []
    for g in range(pairs):
        rows = slice(g * 2 * LANDMARKS, (g + 1) * 2 * LANDMARKS)
        r = dot(p_ref[:, rows], m_ref[rows])
        cols.append((r[:, : 2 * HEAD_DIM] / r[:, 2 * HEAD_DIM :]).astype(BF16))
    per = pairs // 2
    first = jnp.concatenate(cols[:per], axis=1)
    second = jnp.concatenate(cols[per:], axis=1)
    width = own_ref.shape[1]
    for j, (out_ref, wb_ref) in enumerate(((own_ref, wb0_ref), (send_ref, wb1_ref))):
        at = pl.multiple_of((me ^ j) * width, width)
        mixed = dot(first, wo_ref[:, pl.ds(at, width)]) + dot(second, wb_ref[...])
        out_ref[...] = mixed.astype(BF16)


def late_kernel(heads, tok_ref, q_ref, wb_ref, ka_ref, kb_ref, p_ref, kt_ref):
    @pl.when(pl.program_id(0) == 0)
    def _():
        fill_keys(heads, ka_ref, kb_ref, kt_ref)

    weigh(heads, tok_ref, q_ref, wb_ref, kt_ref, p_ref)


def late_weights(start, heads, tokens, queries, other, marks, k_other):
    n, d = tokens.shape
    width = queries.shape[1]
    count = n - start
    tile = math.gcd(count, start)
    base = start // tile
    cols = 2 * heads * LANDMARKS
    return pl.pallas_call(
        functools.partial(late_kernel, heads),
        grid=(count // tile,),
        in_specs=[
            pl.BlockSpec((tile, d), lambda i: (base + i, 0)),
            pl.BlockSpec((tile, width), lambda i: (base + i, 0)),
            pl.BlockSpec((d, width), lambda i: (0, 0)),
            pl.BlockSpec((LANDMARKS, width), lambda i: (0, 1)),
            whole(k_other.shape),
        ],
        out_specs=pl.BlockSpec((tile, cols), lambda i: (i, 0)),
        out_shape=jax.ShapeDtypeStruct((count, cols), BF16),
        scratch_shapes=[pltpu.VMEM((2 * heads, width, LANDMARKS), BF16)],
        compiler_params=params(24),
        cost_estimate=cost(2 * count * (d * width + 2 * heads * 256 * 256), count * 4096),
        name="late",
    )(tokens, queries, other, marks, k_other)


def mix_kernel(first, done, p_ref, wo_ref, wb0_ref, wb1_ref, *refs):
    if first:
        mids, (own_ref, send_ref, m_ref) = refs[:4], refs[-3:]

        @pl.when(pl.program_id(0) == 0)
        def _():
            fill_middle(*mids, m_ref)
    elif done:
        m_ref, a_ref, b_ref, own_ref, send_ref, out_ref, sum_ref, sem = refs
        add_kernel(a_ref, b_ref, sum_ref)
        copy = pltpu.make_async_copy(sum_ref, out_ref.at[pl.ds(0, sum_ref.shape[0])], sem)
        copy.start()
    else:
        m_ref, own_ref, send_ref = refs
    project(p_ref, m_ref, wo_ref, wb0_ref, wb1_ref, own_ref, send_ref)
    if done:
        copy.wait()


def mix(weights, start, count, w_out, other, mids=None, after=None, m=None, done=None, total=0):
    cols = weights.shape[1]
    rows = w_out.shape[0]
    width = other.shape[1]
    skip = (other.shape[0] - 2 * rows) // rows
    tile = count if done else min(1024, count)
    base = start // tile
    args = [weights, w_out, other, other]
    in_specs = [pl.BlockSpec((tile, cols), lambda i: (base + i, 0)), whole(w_out.shape)]
    in_specs += [pl.BlockSpec((rows, width), functools.partial(lambda j, i: (j, 0), skip + j)) for j in range(2)]
    out_specs = [pl.BlockSpec((tile, width), lambda i: (i, 0))] * 2
    out_shape = [jax.ShapeDtypeStruct((count, width), BF16)] * 2
    scratch = []
    if m is None:
        args += [*mids, after]
        in_specs += [whole(x.shape) for x in mids] + [pl.BlockSpec(memory_space=pl.ANY)]
        out_specs += [whole((cols, LANDMARKS))]
        out_shape += [jax.ShapeDtypeStruct((cols, LANDMARKS), BF16)]
    else:
        args += [m]
        in_specs += [whole(m.shape)]
    if done:
        args += list(done)
        in_specs += [whole(x.shape) for x in done]
        out_specs += [pl.BlockSpec(memory_space=pl.ANY)]
        scratch = [pltpu.VMEM(done[0].shape, BF16), pltpu.SemaphoreType.DMA]
        out_shape += [jax.ShapeDtypeStruct((total, width), BF16)]
    return pl.pallas_call(
        functools.partial(mix_kernel, m is None, 1 if done else 0),
        grid=(count // tile,),
        in_specs=in_specs,
        out_specs=out_specs,
        out_shape=out_shape,
        scratch_shapes=scratch,
        compiler_params=params(16),
        cost_estimate=cost(2 * count * (cols * 256 + 4 * rows * width), count * 4096),
        name="mix",
    )(*args)


def add_kernel(own_ref, got_ref, *refs):
    refs[-1][...] = (own_ref[...].astype(F32) + got_ref[...].astype(F32)).astype(BF16)


def add_into(out, own, got, start, total):
    count, width = own.shape
    tile = min(1024, count)
    base = start // tile
    row = pl.BlockSpec((tile, width), lambda i: (i, 0))
    old = [] if out is None else [out]
    return pl.pallas_call(
        add_kernel,
        grid=(count // tile,),
        in_specs=[row, row] + [pl.BlockSpec(memory_space=pl.ANY)] * len(old),
        out_specs=pl.BlockSpec((tile, width), lambda i: (base + i, 0)),
        out_shape=jax.ShapeDtypeStruct((total, width), BF16),
        input_output_aliases={2: 0} if old else {},
        compiler_params=params(4),
        cost_estimate=cost(500_000_000, 6 * own.size),
        name="add",
    )(own, got, *old)


def swap(x, axes, sizes, steps):
    pairs = []
    total = math.prod(sizes)
    for i in range(total):
        rest, at = i, []
        for size in reversed(sizes):
            at.append(rest % size)
            rest //= size
        at = [a ^ s for a, s in zip(reversed(at), steps)]
        to = 0
        for a, size in zip(at, sizes):
            to = to * size + a
        pairs.append((i, to))
    return lax.ppermute(x, axes if len(axes) > 1 else axes[0], pairs)


def gather_doubling(x, n_seq):
    bit = 1
    while bit < n_seq:
        y = swap(x, ("seq",), (n_seq,), (bit,))
        x, *keys = in_order(x, y, bit, 2 * bit == n_seq)
        bit *= 2
    return x, keys[0]


def on_device(n_seq, n_tp, tokens, w_qkv, w_out):
    width = w_out.shape[0]
    heads = width // HEAD_DIM
    far = n_tp // 2

    means, tokens = token_means(tokens, LANDMARKS // n_seq)
    local = local_marks(means, w_qkv)
    send, w_value_t = prepare(w_qkv, w_out, far)
    other = swap(send, ("tp",), (n_tp,), (far,))
    marks, k_marks = gather_doubling(local, n_seq)
    keys = project_rows(tokens, w_qkv, 1)
    queries = project_rows(tokens, w_qkv, 0)
    values_t = project_values(tokens, w_value_t)
    k_other = swap(k_marks, ("tp",), (n_tp,), (far,))

    mine, theirs = block_partials(keys, values_t, marks, heads)
    pair = merge_pair(mine, swap(theirs, ("seq",), (n_seq,), (1,)))
    parts = [pair] + [swap(pair, ("seq",), (n_seq,), (2 * j,)) for j in range(1, n_seq // 2)]
    pinv, early = pseudo_inverse(marks, heads, k_other, tokens, queries, other)
    mid = middle_rows(parts, pinv)
    sizes = (n_seq, n_tp)
    mids = [mid] + [swap(mid, ("seq", "tp"), sizes, s) for s in ((1, 0), (0, far), (1, far))]
    total, done = tokens.shape[0], early.shape[0]
    half = total // 2
    late = late_weights(done, heads, tokens, queries, other, marks, k_other)

    def cross(x):
        return swap(x, ("tp",), (n_tp,), (1,))

    own0, send0, m = mix(early, 0, half, w_out, other, mids=mids, after=late)
    got0 = cross(send0)
    own1, send1 = mix(early, half, done - half, w_out, other, m=m)
    got1 = cross(send1)
    own2, send2, out = mix(late, 0, total - done, w_out, other, m=m, done=(own0, got0), total=total)
    out = add_into(out, own1, got1, half, total)
    return add_into(out, own2, cross(send2), done, total)


def solution(mesh):
    n_seq, n_tp = mesh.shape["seq"], mesh.shape["tp"]
    if n_tp != 4 or n_seq < 2 or n_seq & (n_seq - 1):
        raise ValueError("unsupported mesh")
    in_specs = (P("seq", None), P(None, None, "tp"), P("tp", None))
    return jax.shard_map(
        functools.partial(on_device, n_seq, n_tp),
        mesh=mesh,
        in_specs=in_specs,
        out_specs=P("seq", "tp"),
        check_vma=False,
    )
```

```python
import functools
import math

import jax
import jax.numpy as jnp
from jax import lax
from jax.experimental import pallas as pl
from jax.experimental.pallas import tpu as pltpu
from jax.sharding import PartitionSpec as P

HEAD_DIM = 64
LANDMARKS = 256
NEWTON = 6
FACTOR = HEAD_DIM ** (-0.5) * math.log2(math.e)
PACK_ROWS = HEAD_DIM + 16
TILES = 8


BF16 = jnp.bfloat16
F32 = jnp.float32


def cost(flops, nbytes, trans=0):
    return pl.CostEstimate(flops=flops, bytes_accessed=nbytes, transcendentals=trans)


def params(mib, axes=1):
    return pltpu.CompilerParams(
        dimension_semantics=("arbitrary",) * axes, vmem_limit_bytes=mib * 1024 * 1024
    )


def dot(a, b):
    return jnp.dot(a, b, preferred_element_type=F32)


def dot_nt(a, b):
    return lax.dot_general(a, b, (((1,), (1,)), ((), ())), preferred_element_type=F32)


def split2(x):
    hi = x.astype(BF16)
    lo = (x - hi.astype(F32)).astype(BF16)
    return hi, lo


def dot3(a, b):
    (ah, al), (bh, bl) = a, b
    return dot(jnp.concatenate([ah, ah, al], axis=1), jnp.concatenate([bh, bl, bh], axis=0))


def dot3_nt(a, b):
    (ah, al), (bh, bl) = a, b
    return dot_nt(jnp.concatenate([ah, ah, al], axis=1), jnp.concatenate([bh, bl, bh], axis=1))


def whole(shape):
    zeros = (0,) * len(shape)
    return pl.BlockSpec(shape, lambda *_: zeros)


def means_kernel(segment, count, tok_hbm, out_ref, tok_ref, sems):
    n = tok_ref.shape[0]
    tile = n // count
    copies = []
    for c in range(count):
        rows = pl.ds(c * tile, tile)
        copies.append(pltpu.make_async_copy(tok_hbm.at[rows], tok_ref.at[rows], sems.at[c]))
    for copy in copies:
        copy.start()
    marks = out_ref.shape[0]
    row = lax.broadcasted_iota(jnp.int32, (marks, tile), 0)
    tok = lax.broadcasted_iota(jnp.int32, (marks, tile), 1)
    acc = None
    for c, copy in enumerate(copies):
        at = tok + c * tile
        inside = (at >= row * segment) & (at < (row + 1) * segment)
        pick = jnp.where(inside, 1.0, 0.0).astype(BF16)
        copy.wait()
        part = dot(pick, tok_ref[c * tile : (c + 1) * tile])
        acc = part if acc is None else acc + part
    out_ref[...] = acc * (1.0 / segment)


def token_means(tokens, marks):
    n, d = tokens.shape
    count = 16
    return pl.pallas_call(
        functools.partial(means_kernel, n // marks, count),
        grid=(1,),
        in_specs=[pl.BlockSpec(memory_space=pltpu.HBM)],
        out_specs=[whole((marks, d)), whole((n, d))],
        out_shape=[jax.ShapeDtypeStruct((marks, d), F32), jax.ShapeDtypeStruct((n, d), BF16)],
        scratch_shapes=[pltpu.SemaphoreType.DMA((count,))],
        compiler_params=params(40),
        cost_estimate=cost(6_000_000_000, n * d * 2),
        name="means",
    )(tokens)


def marks_kernel(mean_ref, w_ref, out_ref):
    hi, lo = split2(mean_ref[...])
    width = w_ref.shape[2]
    for c in range(2):
        both = dot(hi, w_ref[c]) + dot(lo, w_ref[c])
        out_ref[:, c * width : (c + 1) * width] = (both * FACTOR).astype(BF16)


def local_marks(means, w_qkv):
    marks, d = means.shape
    width = w_qkv.shape[2]
    return pl.pallas_call(
        marks_kernel,
        grid=(1,),
        in_specs=[whole((marks, d)), pl.BlockSpec((2, d, width), lambda i: (0, 0, 0))],
        out_specs=whole((marks, 2 * width)),
        out_shape=jax.ShapeDtypeStruct((marks, 2 * width), BF16),
        compiler_params=params(6),
        cost_estimate=cost(500_000_000, 1 << 20),
        name="marks",
    )(means, w_qkv)


def prep_kernel(far, wq_ref, wv_ref, wo_ref, send_ref, wvt_ref):
    d, width = send_ref.shape[0] - 2 * wo_ref.shape[0], send_ref.shape[1]
    owner = lax.axis_index("tp") ^ far
    send_ref[:d] = wq_ref[0]
    for j in range(2):
        at = pl.multiple_of((owner ^ j) * width, width)
        send_ref[d + j * width : d + (j + 1) * width] = wo_ref[:, pl.ds(at, width)]
    wvt_ref[...] = wv_ref[0].astype(F32).T.astype(BF16)


def prepare(w_qkv, w_out, far):
    _, d, width = w_qkv.shape
    send = (d + 2 * width, width)
    return pl.pallas_call(
        functools.partial(prep_kernel, far),
        grid=(1,),
        in_specs=[
            pl.BlockSpec((1, d, width), lambda i: (0, 0, 0)),
            pl.BlockSpec((1, d, width), lambda i: (2, 0, 0)),
            whole(w_out.shape),
        ],
        out_specs=[whole(send), whole((width, d))],
        out_shape=[jax.ShapeDtypeStruct(send, BF16), jax.ShapeDtypeStruct((width, d), BF16)],
        compiler_params=params(12),
        cost_estimate=cost(1_000_000_000, 4 << 20),
        name="prep",
    )(w_qkv, w_qkv, w_out)


def order_kernel(bit, x_ref, y_ref, out_ref, *k_refs):
    low = lax.rem(lax.div(lax.axis_index("seq"), bit), 2) == 0
    rows, cols = x_ref.shape
    refs = ((out_ref, 0),) + tuple((r, cols // 2) for r in k_refs)
    for first, a, b in ((low, x_ref, y_ref), (jnp.logical_not(low), y_ref, x_ref)):

        @pl.when(first)
        def _():
            for ref, at in refs:
                ref[:rows] = a[:, at:]
                ref[rows:] = b[:, at:]


def in_order(x, y, bit, split):
    rows, cols = x.shape
    shapes = [(2 * rows, cols)] + [(2 * rows, cols // 2)] * split
    return pl.pallas_call(
        functools.partial(order_kernel, bit),
        grid=(1,),
        in_specs=[whole(x.shape)] * 2,
        out_specs=[whole(s) for s in shapes],
        out_shape=[jax.ShapeDtypeStruct(s, BF16) for s in shapes],
        compiler_params=params(4),
        cost_estimate=cost(100_000_000, 4 * x.size),
        name="order",
    )(x, y)


def rows_kernel(tok_ref, w_ref, out_ref):
    out_ref[...] = dot(tok_ref[...], w_ref[0]).astype(BF16)


def project_rows(tokens, w_qkv, which):
    n, d = tokens.shape
    width = w_qkv.shape[2]
    tile = min(2048, n)
    return pl.pallas_call(
        rows_kernel,
        grid=(n // tile,),
        in_specs=[
            pl.BlockSpec((tile, d), lambda i: (i, 0)),
            pl.BlockSpec((1, d, width), lambda i: (which, 0, 0)),
        ],
        out_specs=pl.BlockSpec((tile, width), lambda i: (i, 0)),
        out_shape=jax.ShapeDtypeStruct((n, width), BF16),
        compiler_params=params(12),
        cost_estimate=cost(2 * n * d * width, n * d * 2 + n * width * 2),
        name="rows",
    )(tokens, w_qkv)


def value_kernel(tok_ref, w_ref, out_ref):
    out_ref[...] = dot_nt(w_ref[...], tok_ref[...]).astype(BF16)


def project_values(tokens, w_value_t):
    n, d = tokens.shape
    width = w_value_t.shape[0]
    tile = min(2048, n)
    return pl.pallas_call(
        value_kernel,
        grid=(n // tile,),
        in_specs=[pl.BlockSpec((tile, d), lambda i: (i, 0)), whole((width, d))],
        out_specs=pl.BlockSpec((width, tile), lambda i: (0, i)),
        out_shape=jax.ShapeDtypeStruct((width, n), BF16),
        compiler_params=params(12),
        cost_estimate=cost(2 * n * d * width, n * d * 2 + n * width * 2),
        name="values",
    )(tokens, w_value_t)


def pack(acc, top, total):
    def three(x):
        hi = x.astype(BF16).astype(F32)
        mid = (x - hi).astype(BF16).astype(F32)
        return hi, mid, x - hi - mid

    rows = three(top) + three(total)
    row = lax.broadcasted_iota(jnp.int32, (PACK_ROWS - HEAD_DIM, acc.shape[1]), 0)
    tail = jnp.zeros(row.shape, F32)
    for i, value in enumerate(rows):
        tail = jnp.where(row == i, value, tail)
    return jnp.concatenate([acc, tail], axis=0).astype(BF16)


def unpack(packed):
    x = packed.astype(F32)
    tail = x[HEAD_DIM:]
    top = tail[0:1] + tail[1:2] + tail[2:3]
    total = tail[3:4] + tail[4:5] + tail[5:6]
    return x[:HEAD_DIM], top, total


def merge(parts):
    parts = [unpack(p) for p in parts]
    top = functools.reduce(jnp.maximum, [p[1] for p in parts])
    factors = [jnp.exp2(p[1] - top) for p in parts]
    acc = sum(p[0] * f for p, f in zip(parts, factors))
    total = sum(p[2] * f for p, f in zip(parts, factors))
    return acc, top, total


def block_kernel(heads, chunk, k_ref, vt_ref, q_ref, mine_ref, theirs_ref, s_ref):
    half = heads // 2
    parity = lax.rem(lax.axis_index("seq"), 2)
    n = k_ref.shape[0]
    queries = q_ref[...].astype(F32).T
    row = lax.broadcasted_iota(jnp.int32, queries.shape, 0)
    order = [(1 - parity) * half + j for j in range(half)] + [parity * half + j for j in range(half)]
    last = None
    for stage in range(heads + 1):
        top = acc = total = None
        if stage < heads:
            low = order[stage] * HEAD_DIM
            inside = (row >= low) & (row < low + HEAD_DIM)
            qt = jnp.where(inside, queries, 0.0).astype(BF16)
        if stage > 0:
            at = pl.multiple_of(order[stage - 1] * HEAD_DIM, HEAD_DIM)
            vt = vt_ref.at[pl.ds(at, HEAD_DIM)]
        for c in range(n // chunk):
            rows = slice(c * chunk, (c + 1) * chunk)
            if stage < heads:
                s = dot(k_ref[rows], qt)
                s_ref[stage % 2, rows] = s
                m = jnp.max(s.reshape(chunk // 8, 8, s.shape[1]), axis=0)
                top = m if top is None else jnp.maximum(top, m)
            if stage > 0:
                e = jnp.exp2(s_ref[(stage - 1) % 2, rows] - last)
                t = jnp.sum(e.reshape(chunk // 8, 8, e.shape[1]), axis=0)
                a = dot(vt[:, rows], e.astype(BF16))
                acc = a if acc is None else acc + a
                total = t if total is None else total + t
        if stage > 0:
            packed = pack(acc, last, jnp.sum(total, axis=0, keepdims=True))
            if stage <= half:
                theirs_ref[stage - 1] = packed
            else:
                mine_ref[stage - 1 - half] = packed
        if stage < heads:
            last = jnp.max(top, axis=0, keepdims=True)


def block_partials(keys, values_t, marks, heads):
    n, width = keys.shape
    half = heads // 2
    shape = (half, PACK_ROWS, LANDMARKS)
    return pl.pallas_call(
        functools.partial(block_kernel, heads, min(1024, n)),
        grid=(1,),
        in_specs=[whole((n, width)), whole((width, n)), pl.BlockSpec((LANDMARKS, width), lambda i: (0, 0))],
        out_specs=[whole(shape), whole(shape)],
        out_shape=[jax.ShapeDtypeStruct(shape, BF16)] * 2,
        scratch_shapes=[pltpu.VMEM((2, n, LANDMARKS), F32)],
        compiler_params=params(24),
        cost_estimate=cost(2 * heads * n * 256 * 256 * 3, n * width * 4, heads * n * LANDMARKS),
        name="block",
    )(keys, values_t, marks)


def merge_kernel(a_ref, b_ref, out_ref):
    for j in range(a_ref.shape[0]):
        out_ref[j] = pack(*merge([a_ref[j], b_ref[j]]))


def merge_pair(a, b):
    return pl.pallas_call(
        merge_kernel,
        in_specs=[whole(a.shape)] * 2,
        out_specs=whole(a.shape),
        grid=(1,),
        out_shape=jax.ShapeDtypeStruct(a.shape, BF16),
        compiler_params=params(4),
        cost_estimate=cost(200_000_000, 4 * a.size),
        name="merge",
    )(a, b)


def newton_kernel(heads, tile, marks_q, marks_k, k_other, tok_ref, q_ref, wb_ref, out_ref, p_ref, x_ref, kt_ref):
    half = heads // 2
    parity = lax.rem(lax.axis_index("seq"), 2)
    size = LANDMARKS
    lane = lax.broadcasted_iota(jnp.int32, marks_q.shape, 1)
    eye = jnp.where(
        lax.broadcasted_iota(jnp.int32, (size, size), 0)
        == lax.broadcasted_iota(jnp.int32, (size, size), 1),
        1.0,
        0.0,
    )
    fill_keys(heads, marks_k, k_other, kt_ref)
    for j in range(half):
        head = parity * half + j
        inside = (lane >= head * HEAD_DIM) & (lane < (head + 1) * HEAD_DIM)
        q = jnp.where(inside, marks_q[...].astype(F32), 0.0).astype(BF16)
        scores = dot_nt(q, marks_k[...]) * (1.0 / FACTOR)
        e = jnp.exp2(scores - jnp.max(scores, axis=1, keepdims=True))
        a = e / jnp.sum(e, axis=1, keepdims=True)
        colmax = jnp.max(jnp.sum(a, axis=0, keepdims=True), axis=1, keepdims=True)
        rowmax = jnp.max(jnp.sum(a, axis=1, keepdims=True), axis=0, keepdims=True)
        z = a.T / (colmax * rowmax)
        out_ref[j] = z
        x_ref[j] = dot3(split2(a), split2(z))

    def weights_of(rows, query, group, h):
        s = dot(query, kt_ref[group * heads + h])
        e = jnp.exp2(s - jnp.max(s, axis=1, keepdims=True))
        at = (group * heads + h) * LANDMARKS
        p_ref[rows, at : at + LANDMARKS] = e.astype(BF16)

    def turn(i, more):
        rows = pl.ds(pl.multiple_of(i * tile, tile), tile)
        half_heads = range(heads // 2), range(heads // 2, heads)
        xs = [x_ref[j] for j in range(half)]
        left = [split2(x) for x in xs]
        square = [dot3(p, p) for p in left]
        other = dot(tok_ref[rows], wb_ref[...]).astype(BF16)
        own = q_ref[rows]
        for h in half_heads[0]:
            weights_of(rows, own, 0, h)
        q = [dot3(split2(square[j]), split2(7.0 * eye - xs[j])) for j in range(half)]
        for h in half_heads[1]:
            weights_of(rows, own, 0, h)
        right = [split2(13.0 * eye - 15.0 * xs[j] + q[j]) for j in range(half)]
        for j in range(half):
            if more:
                x_ref[j] = 0.25 * dot3(left[j], right[j])
            out_ref[j] = 0.25 * dot3(split2(out_ref[j]), right[j])
        for h in range(heads):
            weights_of(rows, other, 1, h)

    def body(i, carry):
        turn(i, True)
        return carry

    lax.fori_loop(0, NEWTON - 1, body, 0)
    turn(NEWTON - 1, False)


def pseudo_inverse(marks, heads, k_other, tokens, queries, other):
    width = marks.shape[1] // 2
    half = heads // 2
    shape = (half, LANDMARKS, LANDMARKS)
    n, d = tokens.shape
    tile = n // TILES
    weights = (NEWTON * tile, 2 * heads * LANDMARKS)
    return pl.pallas_call(
        functools.partial(newton_kernel, heads, tile),
        grid=(1,),
        in_specs=[
            pl.BlockSpec((LANDMARKS, width), lambda i: (0, 0)),
            pl.BlockSpec((LANDMARKS, width), lambda i: (0, 1)),
            whole(k_other.shape),
            whole(tokens.shape),
            whole(queries.shape),
            pl.BlockSpec((d, width), lambda i: (0, 0)),
        ],
        out_specs=[whole(shape), whole(weights)],
        out_shape=[jax.ShapeDtypeStruct(shape, F32), jax.ShapeDtypeStruct(weights, BF16)],
        scratch_shapes=[
            pltpu.VMEM(shape, F32),
            pltpu.VMEM((2 * heads, width, LANDMARKS), BF16),
        ],
        compiler_params=params(16),
        cost_estimate=cost(16_000_000_000, 1 << 20),
        name="newton",
    )(marks, marks, k_other, tokens, queries, other)


def middle_kernel(count, *refs):
    parts, z_ref, out_ref = refs[:count], refs[count], refs[count + 1]
    for j in range(z_ref.shape[0]):
        acc, _, total = merge([p[j] for p in parts])
        out_ref[j] = dot3_nt(split2(acc / total), split2(z_ref[j])).astype(BF16)


def middle_rows(parts, pinv):
    half = pinv.shape[0]
    shape = (half, HEAD_DIM, LANDMARKS)
    return pl.pallas_call(
        functools.partial(middle_kernel, len(parts)),
        grid=(1,),
        in_specs=[whole(p.shape) for p in parts] + [whole(pinv.shape)],
        out_specs=whole(shape),
        out_shape=jax.ShapeDtypeStruct(shape, BF16),
        compiler_params=params(8),
        cost_estimate=cost(1_000_000_000, 1 << 20),
        name="middle",
    )(*parts, pinv)


def fill_keys(heads, ka_ref, kb_ref, kt_ref):
    for g, ref in enumerate((ka_ref, kb_ref)):
        kt = ref[...].astype(F32).T
        row = lax.broadcasted_iota(jnp.int32, kt.shape, 0)
        for h in range(heads):
            inside = (row >= h * HEAD_DIM) & (row < (h + 1) * HEAD_DIM)
            kt_ref[g * heads + h] = jnp.where(inside, kt, 0.0).astype(BF16)


def fill_middle(mine_ref, x_ref, y_ref, xy_ref, m_ref):
    parity = lax.rem(lax.axis_index("seq"), 2)
    half = mine_ref.shape[0]
    zeros = jnp.zeros((HEAD_DIM, LANDMARKS), F32)
    ones = jnp.ones((HEAD_DIM, LANDMARKS), F32)
    for group, (a, b) in enumerate(((mine_ref, x_ref), (y_ref, xy_ref))):
        for side in range(2):
            for j in range(half):
                mid = jnp.where(parity == side, a[j].astype(F32), b[j].astype(F32))
                blocks = [zeros, zeros, zeros, zeros]
                blocks[j % 2] = mid
                blocks[2 + j % 2] = ones
                full = jnp.concatenate(blocks, axis=0).T.astype(BF16)
                at = ((group * 2 + side) * half + j) * LANDMARKS
                m_ref[at : at + LANDMARKS] = full


def weigh(heads, tok_ref, q_ref, wb_ref, kt_ref, p_ref):
    for g in range(2):
        q = q_ref[...] if g == 0 else dot(tok_ref[...], wb_ref[...]).astype(BF16)
        for h in range(heads):
            s = dot(q, kt_ref[g * heads + h])
            e = jnp.exp2(s - jnp.max(s, axis=1, keepdims=True))
            at = (g * heads + h) * LANDMARKS
            p_ref[:, at : at + LANDMARKS] = e.astype(BF16)


def project(p_ref, m_ref, wo_ref, wb0_ref, wb1_ref, own_ref, send_ref):
    me = lax.axis_index("tp")
    pairs = m_ref.shape[0] // (2 * LANDMARKS)
    cols = []
    for g in range(pairs):
        rows = slice(g * 2 * LANDMARKS, (g + 1) * 2 * LANDMARKS)
        r = dot(p_ref[:, rows], m_ref[rows])
        cols.append((r[:, : 2 * HEAD_DIM] / r[:, 2 * HEAD_DIM :]).astype(BF16))
    per = pairs // 2
    first = jnp.concatenate(cols[:per], axis=1)
    second = jnp.concatenate(cols[per:], axis=1)
    width = own_ref.shape[1]
    for j, (out_ref, wb_ref) in enumerate(((own_ref, wb0_ref), (send_ref, wb1_ref))):
        at = pl.multiple_of((me ^ j) * width, width)
        mixed = dot(first, wo_ref[:, pl.ds(at, width)]) + dot(second, wb_ref[...])
        out_ref[...] = mixed.astype(BF16)


def late_kernel(heads, tok_ref, q_ref, wb_ref, ka_ref, kb_ref, p_ref, kt_ref):
    @pl.when(pl.program_id(0) == 0)
    def _():
        fill_keys(heads, ka_ref, kb_ref, kt_ref)

    weigh(heads, tok_ref, q_ref, wb_ref, kt_ref, p_ref)


def late_weights(start, heads, tokens, queries, other, marks, k_other):
    n, d = tokens.shape
    width = queries.shape[1]
    count = n - start
    tile = math.gcd(count, start)
    base = start // tile
    cols = 2 * heads * LANDMARKS
    return pl.pallas_call(
        functools.partial(late_kernel, heads),
        grid=(count // tile,),
        in_specs=[
            pl.BlockSpec((tile, d), lambda i: (base + i, 0)),
            pl.BlockSpec((tile, width), lambda i: (base + i, 0)),
            pl.BlockSpec((d, width), lambda i: (0, 0)),
            pl.BlockSpec((LANDMARKS, width), lambda i: (0, 1)),
            whole(k_other.shape),
        ],
        out_specs=pl.BlockSpec((tile, cols), lambda i: (i, 0)),
        out_shape=jax.ShapeDtypeStruct((count, cols), BF16),
        scratch_shapes=[pltpu.VMEM((2 * heads, width, LANDMARKS), BF16)],
        compiler_params=params(24),
        cost_estimate=cost(2 * count * (d * width + 2 * heads * 256 * 256), count * 4096),
        name="late",
    )(tokens, queries, other, marks, k_other)


def mix_kernel(first, done, p_ref, wo_ref, wb0_ref, wb1_ref, *refs):
    if first:
        mids, (own_ref, send_ref, m_ref) = refs[:4], refs[-3:]

        @pl.when(pl.program_id(0) == 0)
        def _():
            fill_middle(*mids, m_ref)
    elif done:
        m_ref, a_ref, b_ref, own_ref, send_ref, out_ref, sum_ref, sem = refs
        count = sum_ref.shape[0]
        tile = count // 8

        def add_rows(i, carry):
            rows = pl.ds(pl.multiple_of(i * tile, tile), tile)
            sum_ref[rows] = (a_ref[rows].astype(F32) + b_ref[rows].astype(F32)).astype(BF16)
            return carry

        lax.fori_loop(0, 8, add_rows, 0)
        copy = pltpu.make_async_copy(sum_ref, out_ref.at[pl.ds(0, count)], sem)
        copy.start()
    else:
        m_ref, own_ref, send_ref = refs
    project(p_ref, m_ref, wo_ref, wb0_ref, wb1_ref, own_ref, send_ref)
    if done:
        copy.wait()


def mix(weights, start, count, w_out, other, mids=None, after=None, m=None, done=None, total=0):
    cols = weights.shape[1]
    rows = w_out.shape[0]
    width = other.shape[1]
    skip = (other.shape[0] - 2 * rows) // rows
    tile = count if done else min(1024, count)
    base = start // tile
    args = [weights, w_out, other, other]
    in_specs = [pl.BlockSpec((tile, cols), lambda i: (base + i, 0)), whole(w_out.shape)]
    in_specs += [pl.BlockSpec((rows, width), functools.partial(lambda j, i: (j, 0), skip + j)) for j in range(2)]
    out_specs = [pl.BlockSpec((tile, width), lambda i: (i, 0))] * 2
    out_shape = [jax.ShapeDtypeStruct((count, width), BF16)] * 2
    scratch = []
    if m is None:
        args += [*mids, after]
        in_specs += [whole(x.shape) for x in mids] + [pl.BlockSpec(memory_space=pl.ANY)]
        out_specs += [whole((cols, LANDMARKS))]
        out_shape += [jax.ShapeDtypeStruct((cols, LANDMARKS), BF16)]
    else:
        args += [m]
        in_specs += [whole(m.shape)]
    if done:
        args += list(done)
        in_specs += [whole(x.shape) for x in done]
        out_specs += [pl.BlockSpec(memory_space=pl.ANY)]
        scratch = [pltpu.VMEM(done[0].shape, BF16), pltpu.SemaphoreType.DMA]
        out_shape += [jax.ShapeDtypeStruct((total, width), BF16)]
    return pl.pallas_call(
        functools.partial(mix_kernel, m is None, 1 if done else 0),
        grid=(count // tile,),
        in_specs=in_specs,
        out_specs=out_specs,
        out_shape=out_shape,
        scratch_shapes=scratch,
        compiler_params=params(16),
        cost_estimate=cost(2 * count * (cols * 256 + 4 * rows * width), count * 4096),
        name="mix",
    )(*args)


def add_kernel(own_ref, got_ref, *refs):
    refs[-1][...] = (own_ref[...].astype(F32) + got_ref[...].astype(F32)).astype(BF16)


def add_into(out, own, got, start, total):
    count, width = own.shape
    tile = min(1024, count)
    base = start // tile
    row = pl.BlockSpec((tile, width), lambda i: (i, 0))
    old = [] if out is None else [out]
    return pl.pallas_call(
        add_kernel,
        grid=(count // tile,),
        in_specs=[row, row] + [pl.BlockSpec(memory_space=pl.ANY)] * len(old),
        out_specs=pl.BlockSpec((tile, width), lambda i: (base + i, 0)),
        out_shape=jax.ShapeDtypeStruct((total, width), BF16),
        input_output_aliases={2: 0} if old else {},
        compiler_params=params(4),
        cost_estimate=cost(500_000_000, 6 * own.size),
        name="add",
    )(own, got, *old)


def swap(x, axes, sizes, steps):
    pairs = []
    total = math.prod(sizes)
    for i in range(total):
        rest, at = i, []
        for size in reversed(sizes):
            at.append(rest % size)
            rest //= size
        at = [a ^ s for a, s in zip(reversed(at), steps)]
        to = 0
        for a, size in zip(at, sizes):
            to = to * size + a
        pairs.append((i, to))
    return lax.ppermute(x, axes if len(axes) > 1 else axes[0], pairs)


def gather_doubling(x, n_seq):
    bit = 1
    while bit < n_seq:
        y = swap(x, ("seq",), (n_seq,), (bit,))
        x, *keys = in_order(x, y, bit, 2 * bit == n_seq)
        bit *= 2
    return x, keys[0]


def on_device(n_seq, n_tp, tokens, w_qkv, w_out):
    width = w_out.shape[0]
    heads = width // HEAD_DIM
    far = n_tp // 2

    means, tokens = token_means(tokens, LANDMARKS // n_seq)
    local = local_marks(means, w_qkv)
    send, w_value_t = prepare(w_qkv, w_out, far)
    other = swap(send, ("tp",), (n_tp,), (far,))
    marks, k_marks = gather_doubling(local, n_seq)
    keys = project_rows(tokens, w_qkv, 1)
    queries = project_rows(tokens, w_qkv, 0)
    values_t = project_values(tokens, w_value_t)
    k_other = swap(k_marks, ("tp",), (n_tp,), (far,))

    mine, theirs = block_partials(keys, values_t, marks, heads)
    pair = merge_pair(mine, swap(theirs, ("seq",), (n_seq,), (1,)))
    parts = [pair] + [swap(pair, ("seq",), (n_seq,), (2 * j,)) for j in reversed(range(1, n_seq // 2))]
    pinv, early = pseudo_inverse(marks, heads, k_other, tokens, queries, other)
    mid = middle_rows(parts, pinv)
    sizes = (n_seq, n_tp)
    mids = [mid] + [swap(mid, ("seq", "tp"), sizes, s) for s in ((1, 0), (0, far), (1, far))]
    total, done = tokens.shape[0], early.shape[0]
    half = total // 2
    late = late_weights(done, heads, tokens, queries, other, marks, k_other)

    def cross(x):
        return swap(x, ("tp",), (n_tp,), (1,))

    own0, send0, m = mix(early, 0, half, w_out, other, mids=mids, after=late)
    got0 = cross(send0)
    own1, send1 = mix(early, half, done - half, w_out, other, m=m)
    got1 = cross(send1)
    own2, send2, out = mix(late, 0, total - done, w_out, other, m=m, done=(own0, got0), total=total)
    out = add_into(out, own1, got1, half, total)
    return add_into(out, own2, cross(send2), done, total)


def solution(mesh):
    n_seq, n_tp = mesh.shape["seq"], mesh.shape["tp"]
    if n_tp != 4 or n_seq < 2 or n_seq & (n_seq - 1):
        raise ValueError("unsupported mesh")
    in_specs = (P("seq", None), P(None, None, "tp"), P("tp", None))
    return jax.shard_map(
        functools.partial(on_device, n_seq, n_tp),
        mesh=mesh,
        in_specs=in_specs,
        out_specs=P("seq", "tp"),
        check_vma=False,
    )
```

```python
import functools
import math

import jax
import jax.numpy as jnp
from jax import lax
from jax.experimental import pallas as pl
from jax.experimental.pallas import tpu as pltpu
from jax.sharding import PartitionSpec as P

HEAD_DIM = 64
LANDMARKS = 256
NEWTON = 6
FACTOR = HEAD_DIM ** (-0.5) * math.log2(math.e)
PACK_ROWS = HEAD_DIM + 16
TILES = 8


BF16 = jnp.bfloat16
F32 = jnp.float32


def cost(flops, nbytes, trans=0):
    return pl.CostEstimate(flops=flops, bytes_accessed=nbytes, transcendentals=trans)


def params(mib, axes=1):
    return pltpu.CompilerParams(
        dimension_semantics=("arbitrary",) * axes, vmem_limit_bytes=mib * 1024 * 1024
    )


def dot(a, b):
    return jnp.dot(a, b, preferred_element_type=F32)


def dot_nt(a, b):
    return lax.dot_general(a, b, (((1,), (1,)), ((), ())), preferred_element_type=F32)


def split2(x):
    hi = x.astype(BF16)
    lo = (x - hi.astype(F32)).astype(BF16)
    return hi, lo


def dot3(a, b):
    (ah, al), (bh, bl) = a, b
    return dot(jnp.concatenate([ah, ah, al], axis=1), jnp.concatenate([bh, bl, bh], axis=0))


def dot3_nt(a, b):
    (ah, al), (bh, bl) = a, b
    return dot_nt(jnp.concatenate([ah, ah, al], axis=1), jnp.concatenate([bh, bl, bh], axis=1))


def whole(shape):
    zeros = (0,) * len(shape)
    return pl.BlockSpec(shape, lambda *_: zeros)


def means_kernel(segment, count, tok_hbm, out_ref, tok_ref, sems):
    n = tok_ref.shape[0]
    tile = n // count
    copies = []
    for c in range(count):
        rows = pl.ds(c * tile, tile)
        copies.append(pltpu.make_async_copy(tok_hbm.at[rows], tok_ref.at[rows], sems.at[c]))
    for copy in copies:
        copy.start()
    marks = out_ref.shape[0]
    row = lax.broadcasted_iota(jnp.int32, (marks, tile), 0)
    tok = lax.broadcasted_iota(jnp.int32, (marks, tile), 1)
    acc = None
    for c, copy in enumerate(copies):
        at = tok + c * tile
        inside = (at >= row * segment) & (at < (row + 1) * segment)
        pick = jnp.where(inside, 1.0, 0.0).astype(BF16)
        copy.wait()
        part = dot(pick, tok_ref[c * tile : (c + 1) * tile])
        acc = part if acc is None else acc + part
    out_ref[...] = acc * (1.0 / segment)


def token_means(tokens, marks):
    n, d = tokens.shape
    count = 16
    return pl.pallas_call(
        functools.partial(means_kernel, n // marks, count),
        grid=(1,),
        in_specs=[pl.BlockSpec(memory_space=pltpu.HBM)],
        out_specs=[whole((marks, d)), whole((n, d))],
        out_shape=[jax.ShapeDtypeStruct((marks, d), F32), jax.ShapeDtypeStruct((n, d), BF16)],
        scratch_shapes=[pltpu.SemaphoreType.DMA((count,))],
        compiler_params=params(40),
        cost_estimate=cost(6_000_000_000, n * d * 2),
        name="means",
    )(tokens)


def marks_kernel(mean_ref, w_ref, out_ref):
    hi, lo = split2(mean_ref[...])
    width = w_ref.shape[2]
    for c in range(2):
        both = dot(hi, w_ref[c]) + dot(lo, w_ref[c])
        out_ref[:, c * width : (c + 1) * width] = (both * FACTOR).astype(BF16)


def local_marks(means, w_qkv):
    marks, d = means.shape
    width = w_qkv.shape[2]
    return pl.pallas_call(
        marks_kernel,
        grid=(1,),
        in_specs=[whole((marks, d)), pl.BlockSpec((2, d, width), lambda i: (0, 0, 0))],
        out_specs=whole((marks, 2 * width)),
        out_shape=jax.ShapeDtypeStruct((marks, 2 * width), BF16),
        compiler_params=params(6),
        cost_estimate=cost(500_000_000, 1 << 20),
        name="marks",
    )(means, w_qkv)


def prep_kernel(far, wq_ref, wv_ref, wo_ref, send_ref, wvt_ref):
    d, width = send_ref.shape[0] - 2 * wo_ref.shape[0], send_ref.shape[1]
    owner = lax.axis_index("tp") ^ far
    send_ref[:d] = wq_ref[0]
    for j in range(2):
        at = pl.multiple_of((owner ^ j) * width, width)
        send_ref[d + j * width : d + (j + 1) * width] = wo_ref[:, pl.ds(at, width)]
    wvt_ref[...] = wv_ref[0].astype(F32).T.astype(BF16)


def prepare(w_qkv, w_out, far):
    _, d, width = w_qkv.shape
    send = (d + 2 * width, width)
    return pl.pallas_call(
        functools.partial(prep_kernel, far),
        grid=(1,),
        in_specs=[
            pl.BlockSpec((1, d, width), lambda i: (0, 0, 0)),
            pl.BlockSpec((1, d, width), lambda i: (2, 0, 0)),
            whole(w_out.shape),
        ],
        out_specs=[whole(send), whole((width, d))],
        out_shape=[jax.ShapeDtypeStruct(send, BF16), jax.ShapeDtypeStruct((width, d), BF16)],
        compiler_params=params(12),
        cost_estimate=cost(1_000_000_000, 4 << 20),
        name="prep",
    )(w_qkv, w_qkv, w_out)


def order_kernel(bit, x_ref, y_ref, out_ref, *k_refs):
    low = lax.rem(lax.div(lax.axis_index("seq"), bit), 2) == 0
    rows, cols = x_ref.shape
    refs = ((out_ref, 0),) + tuple((r, cols // 2) for r in k_refs)
    for first, a, b in ((low, x_ref, y_ref), (jnp.logical_not(low), y_ref, x_ref)):

        @pl.when(first)
        def _():
            for ref, at in refs:
                ref[:rows] = a[:, at:]
                ref[rows:] = b[:, at:]


def in_order(x, y, bit, split):
    rows, cols = x.shape
    shapes = [(2 * rows, cols)] + [(2 * rows, cols // 2)] * split
    return pl.pallas_call(
        functools.partial(order_kernel, bit),
        grid=(1,),
        in_specs=[whole(x.shape)] * 2,
        out_specs=[whole(s) for s in shapes],
        out_shape=[jax.ShapeDtypeStruct(s, BF16) for s in shapes],
        compiler_params=params(4),
        cost_estimate=cost(100_000_000, 4 * x.size),
        name="order",
    )(x, y)


def rows_kernel(tok_ref, w_ref, out_ref):
    out_ref[...] = dot(tok_ref[...], w_ref[0]).astype(BF16)


def project_rows(tokens, w_qkv, which):
    n, d = tokens.shape
    width = w_qkv.shape[2]
    tile = min(2048, n)
    return pl.pallas_call(
        rows_kernel,
        grid=(n // tile,),
        in_specs=[
            pl.BlockSpec((tile, d), lambda i: (i, 0)),
            pl.BlockSpec((1, d, width), lambda i: (which, 0, 0)),
        ],
        out_specs=pl.BlockSpec((tile, width), lambda i: (i, 0)),
        out_shape=jax.ShapeDtypeStruct((n, width), BF16),
        compiler_params=params(12),
        cost_estimate=cost(2 * n * d * width, n * d * 2 + n * width * 2),
        name="rows",
    )(tokens, w_qkv)


def value_kernel(tok_ref, w_ref, out_ref):
    out_ref[...] = dot_nt(w_ref[...], tok_ref[...]).astype(BF16)


def project_values(tokens, w_value_t):
    n, d = tokens.shape
    width = w_value_t.shape[0]
    tile = min(2048, n)
    return pl.pallas_call(
        value_kernel,
        grid=(n // tile,),
        in_specs=[pl.BlockSpec((tile, d), lambda i: (i, 0)), whole((width, d))],
        out_specs=pl.BlockSpec((width, tile), lambda i: (0, i)),
        out_shape=jax.ShapeDtypeStruct((width, n), BF16),
        compiler_params=params(12),
        cost_estimate=cost(2 * n * d * width, n * d * 2 + n * width * 2),
        name="values",
    )(tokens, w_value_t)


def pack(acc, top, total):
    def three(x):
        hi = x.astype(BF16).astype(F32)
        mid = (x - hi).astype(BF16).astype(F32)
        return hi, mid, x - hi - mid

    rows = three(top) + three(total)
    row = lax.broadcasted_iota(jnp.int32, (PACK_ROWS - HEAD_DIM, acc.shape[1]), 0)
    tail = jnp.zeros(row.shape, F32)
    for i, value in enumerate(rows):
        tail = jnp.where(row == i, value, tail)
    return jnp.concatenate([acc, tail], axis=0).astype(BF16)


def unpack(packed):
    x = packed.astype(F32)
    tail = x[HEAD_DIM:]
    top = tail[0:1] + tail[1:2] + tail[2:3]
    total = tail[3:4] + tail[4:5] + tail[5:6]
    return x[:HEAD_DIM], top, total


def merge(parts):
    parts = [unpack(p) for p in parts]
    top = functools.reduce(jnp.maximum, [p[1] for p in parts])
    factors = [jnp.exp2(p[1] - top) for p in parts]
    acc = sum(p[0] * f for p, f in zip(parts, factors))
    total = sum(p[2] * f for p, f in zip(parts, factors))
    return acc, top, total


def block_kernel(heads, chunk, k_ref, vt_ref, q_ref, mine_ref, theirs_ref, s_ref):
    half = heads // 2
    parity = lax.rem(lax.axis_index("seq"), 2)
    n = k_ref.shape[0]
    queries = q_ref[...].astype(F32).T
    row = lax.broadcasted_iota(jnp.int32, queries.shape, 0)
    order = [(1 - parity) * half + j for j in range(half)] + [parity * half + j for j in range(half)]
    last = None
    for stage in range(heads + 1):
        top = acc = total = None
        if stage < heads:
            low = order[stage] * HEAD_DIM
            inside = (row >= low) & (row < low + HEAD_DIM)
            qt = jnp.where(inside, queries, 0.0).astype(BF16)
        if stage > 0:
            at = pl.multiple_of(order[stage - 1] * HEAD_DIM, HEAD_DIM)
            vt = vt_ref.at[pl.ds(at, HEAD_DIM)]
        for c in range(n // chunk):
            rows = slice(c * chunk, (c + 1) * chunk)
            if stage < heads:
                s = dot(k_ref[rows], qt)
                s_ref[stage % 2, rows] = s
                m = jnp.max(s.reshape(chunk // 8, 8, s.shape[1]), axis=0)
                top = m if top is None else jnp.maximum(top, m)
            if stage > 0:
                e = jnp.exp2(s_ref[(stage - 1) % 2, rows] - last)
                t = jnp.sum(e.reshape(chunk // 8, 8, e.shape[1]), axis=0)
                a = dot(vt[:, rows], e.astype(BF16))
                acc = a if acc is None else acc + a
                total = t if total is None else total + t
        if stage > 0:
            packed = pack(acc, last, jnp.sum(total, axis=0, keepdims=True))
            if stage <= half:
                theirs_ref[stage - 1] = packed
            else:
                mine_ref[stage - 1 - half] = packed
        if stage < heads:
            last = jnp.max(top, axis=0, keepdims=True)


def block_partials(keys, values_t, marks, heads):
    n, width = keys.shape
    half = heads // 2
    shape = (half, PACK_ROWS, LANDMARKS)
    return pl.pallas_call(
        functools.partial(block_kernel, heads, min(1024, n)),
        grid=(1,),
        in_specs=[whole((n, width)), whole((width, n)), pl.BlockSpec((LANDMARKS, width), lambda i: (0, 0))],
        out_specs=[whole(shape), whole(shape)],
        out_shape=[jax.ShapeDtypeStruct(shape, BF16)] * 2,
        scratch_shapes=[pltpu.VMEM((2, n, LANDMARKS), F32)],
        compiler_params=params(24),
        cost_estimate=cost(2 * heads * n * 256 * 256 * 3, n * width * 4, heads * n * LANDMARKS),
        name="block",
    )(keys, values_t, marks)


def merge_kernel(a_ref, b_ref, out_ref):
    for j in range(a_ref.shape[0]):
        out_ref[j] = pack(*merge([a_ref[j], b_ref[j]]))


def merge_pair(a, b):
    return pl.pallas_call(
        merge_kernel,
        in_specs=[whole(a.shape)] * 2,
        out_specs=whole(a.shape),
        grid=(1,),
        out_shape=jax.ShapeDtypeStruct(a.shape, BF16),
        compiler_params=params(4),
        cost_estimate=cost(200_000_000, 4 * a.size),
        name="merge",
    )(a, b)


def newton_kernel(heads, tile, marks_q, marks_k, k_other, tok_ref, q_ref, wb_ref, out_ref, p_ref, x_ref, kt_ref):
    half = heads // 2
    parity = lax.rem(lax.axis_index("seq"), 2)
    size = LANDMARKS
    lane = lax.broadcasted_iota(jnp.int32, marks_q.shape, 1)
    eye = jnp.where(
        lax.broadcasted_iota(jnp.int32, (size, size), 0)
        == lax.broadcasted_iota(jnp.int32, (size, size), 1),
        1.0,
        0.0,
    )
    fill_keys(heads, marks_k, k_other, kt_ref)
    for j in range(half):
        head = parity * half + j
        inside = (lane >= head * HEAD_DIM) & (lane < (head + 1) * HEAD_DIM)
        q = jnp.where(inside, marks_q[...].astype(F32), 0.0).astype(BF16)
        scores = dot_nt(q, marks_k[...]) * (1.0 / FACTOR)
        e = jnp.exp2(scores - jnp.max(scores, axis=1, keepdims=True))
        a = e / jnp.sum(e, axis=1, keepdims=True)
        colmax = jnp.max(jnp.sum(a, axis=0, keepdims=True), axis=1, keepdims=True)
        rowmax = jnp.max(jnp.sum(a, axis=1, keepdims=True), axis=0, keepdims=True)
        z = a.T / (colmax * rowmax)
        out_ref[j] = z
        x_ref[j] = dot3(split2(a), split2(z))

    def weights_of(rows, query, group, h):
        s = dot(query, kt_ref[group * heads + h])
        e = jnp.exp2(s - jnp.max(s, axis=1, keepdims=True))
        at = (group * heads + h) * LANDMARKS
        p_ref[rows, at : at + LANDMARKS] = e.astype(BF16)

    def turn(i, more):
        rows = pl.ds(pl.multiple_of(i * tile, tile), tile)
        half_heads = range(heads // 2), range(heads // 2, heads)
        xs = [x_ref[j] for j in range(half)]
        left = [split2(x) for x in xs]
        square = [dot3(p, p) for p in left]
        other = dot(tok_ref[rows], wb_ref[...]).astype(BF16)
        own = q_ref[rows]
        for h in half_heads[0]:
            weights_of(rows, own, 0, h)
        q = [dot3(split2(square[j]), split2(7.0 * eye - xs[j])) for j in range(half)]
        for h in half_heads[1]:
            weights_of(rows, own, 0, h)
        right = [split2(13.0 * eye - 15.0 * xs[j] + q[j]) for j in range(half)]
        for j in range(half):
            if more:
                x_ref[j] = 0.25 * dot3(left[j], right[j])
            out_ref[j] = 0.25 * dot3(split2(out_ref[j]), right[j])
        for h in range(heads):
            weights_of(rows, other, 1, h)

    def body(i, carry):
        turn(i, True)
        return carry

    lax.fori_loop(0, NEWTON - 1, body, 0)
    turn(NEWTON - 1, False)


def pseudo_inverse(marks, heads, k_other, tokens, queries, other):
    width = marks.shape[1] // 2
    half = heads // 2
    shape = (half, LANDMARKS, LANDMARKS)
    n, d = tokens.shape
    tile = n // TILES
    weights = (NEWTON * tile, 2 * heads * LANDMARKS)
    return pl.pallas_call(
        functools.partial(newton_kernel, heads, tile),
        grid=(1,),
        in_specs=[
            pl.BlockSpec((LANDMARKS, width), lambda i: (0, 0)),
            pl.BlockSpec((LANDMARKS, width), lambda i: (0, 1)),
            whole(k_other.shape),
            whole(tokens.shape),
            whole(queries.shape),
            pl.BlockSpec((d, width), lambda i: (0, 0)),
        ],
        out_specs=[whole(shape), whole(weights)],
        out_shape=[jax.ShapeDtypeStruct(shape, F32), jax.ShapeDtypeStruct(weights, BF16)],
        scratch_shapes=[
            pltpu.VMEM(shape, F32),
            pltpu.VMEM((2 * heads, width, LANDMARKS), BF16),
        ],
        compiler_params=params(16),
        cost_estimate=cost(16_000_000_000, 1 << 20),
        name="newton",
    )(marks, marks, k_other, tokens, queries, other)


def middle_kernel(count, *refs):
    parts, z_ref, out_ref = refs[:count], refs[count], refs[count + 1]
    for j in range(z_ref.shape[0]):
        acc, _, total = merge([p[j] for p in parts])
        out_ref[j] = dot3_nt(split2(acc / total), split2(z_ref[j])).astype(BF16)


def middle_rows(parts, pinv):
    half = pinv.shape[0]
    shape = (half, HEAD_DIM, LANDMARKS)
    return pl.pallas_call(
        functools.partial(middle_kernel, len(parts)),
        grid=(1,),
        in_specs=[whole(p.shape) for p in parts] + [whole(pinv.shape)],
        out_specs=whole(shape),
        out_shape=jax.ShapeDtypeStruct(shape, BF16),
        compiler_params=params(8),
        cost_estimate=cost(1_000_000_000, 1 << 20),
        name="middle",
    )(*parts, pinv)


def fill_keys(heads, ka_ref, kb_ref, kt_ref):
    for g, ref in enumerate((ka_ref, kb_ref)):
        kt = ref[...].astype(F32).T
        row = lax.broadcasted_iota(jnp.int32, kt.shape, 0)
        for h in range(heads):
            inside = (row >= h * HEAD_DIM) & (row < (h + 1) * HEAD_DIM)
            kt_ref[g * heads + h] = jnp.where(inside, kt, 0.0).astype(BF16)


def fill_middle(mine_ref, x_ref, y_ref, xy_ref, m_ref):
    parity = lax.rem(lax.axis_index("seq"), 2)
    half = mine_ref.shape[0]
    zeros = jnp.zeros((HEAD_DIM, LANDMARKS), F32)
    ones = jnp.ones((HEAD_DIM, LANDMARKS), F32)
    for group, (a, b) in enumerate(((mine_ref, x_ref), (y_ref, xy_ref))):
        for side in range(2):
            for j in range(half):
                mid = jnp.where(parity == side, a[j].astype(F32), b[j].astype(F32))
                blocks = [zeros, zeros, zeros, zeros]
                blocks[j % 2] = mid
                blocks[2 + j % 2] = ones
                full = jnp.concatenate(blocks, axis=0).T.astype(BF16)
                at = ((group * 2 + side) * half + j) * LANDMARKS
                m_ref[at : at + LANDMARKS] = full


def weigh(heads, tok_ref, q_ref, wb_ref, kt_ref, p_ref):
    for g in range(2):
        q = q_ref[...] if g == 0 else dot(tok_ref[...], wb_ref[...]).astype(BF16)
        for h in range(heads):
            s = dot(q, kt_ref[g * heads + h])
            e = jnp.exp2(s - jnp.max(s, axis=1, keepdims=True))
            at = (g * heads + h) * LANDMARKS
            p_ref[:, at : at + LANDMARKS] = e.astype(BF16)


def project(p_ref, m_ref, wo_ref, wb0_ref, wb1_ref, own_ref, send_ref):
    me = lax.axis_index("tp")
    pairs = m_ref.shape[0] // (2 * LANDMARKS)
    cols = []
    for g in range(pairs):
        rows = slice(g * 2 * LANDMARKS, (g + 1) * 2 * LANDMARKS)
        r = dot(p_ref[:, rows], m_ref[rows])
        cols.append((r[:, : 2 * HEAD_DIM] / r[:, 2 * HEAD_DIM :]).astype(BF16))
    per = pairs // 2
    first = jnp.concatenate(cols[:per], axis=1)
    second = jnp.concatenate(cols[per:], axis=1)
    width = own_ref.shape[1]
    for j, (out_ref, wb_ref) in enumerate(((own_ref, wb0_ref), (send_ref, wb1_ref))):
        at = pl.multiple_of((me ^ j) * width, width)
        mixed = dot(first, wo_ref[:, pl.ds(at, width)]) + dot(second, wb_ref[...])
        out_ref[...] = mixed.astype(BF16)


def late_kernel(heads, tok_ref, q_ref, wb_ref, ka_ref, kb_ref, p_ref, kt_ref):
    @pl.when(pl.program_id(0) == 0)
    def _():
        fill_keys(heads, ka_ref, kb_ref, kt_ref)

    weigh(heads, tok_ref, q_ref, wb_ref, kt_ref, p_ref)


def late_weights(start, heads, tokens, queries, other, marks, k_other):
    n, d = tokens.shape
    width = queries.shape[1]
    count = n - start
    tile = math.gcd(count, start)
    base = start // tile
    cols = 2 * heads * LANDMARKS
    return pl.pallas_call(
        functools.partial(late_kernel, heads),
        grid=(count // tile,),
        in_specs=[
            pl.BlockSpec((tile, d), lambda i: (base + i, 0)),
            pl.BlockSpec((tile, width), lambda i: (base + i, 0)),
            pl.BlockSpec((d, width), lambda i: (0, 0)),
            pl.BlockSpec((LANDMARKS, width), lambda i: (0, 1)),
            whole(k_other.shape),
        ],
        out_specs=pl.BlockSpec((tile, cols), lambda i: (i, 0)),
        out_shape=jax.ShapeDtypeStruct((count, cols), BF16),
        scratch_shapes=[pltpu.VMEM((2 * heads, width, LANDMARKS), BF16)],
        compiler_params=params(24),
        cost_estimate=cost(2 * count * (d * width + 2 * heads * 256 * 256), count * 4096),
        name="late",
    )(tokens, queries, other, marks, k_other)


def mix_kernel(first, done, p_ref, wo_ref, wb0_ref, wb1_ref, *refs):
    if first:
        mids, (own_ref, send_ref, m_ref) = refs[:4], refs[-3:]

        @pl.when(pl.program_id(0) == 0)
        def _():
            fill_middle(*mids, m_ref)
    elif done:
        m_ref, a_ref, b_ref, own_ref, send_ref, out_ref, sum_ref, sem = refs
        count = sum_ref.shape[0]
        tile = count // 8

        def add_rows(i, carry):
            rows = pl.ds(pl.multiple_of(i * tile, tile), tile)
            sum_ref[rows] = (a_ref[rows].astype(F32) + b_ref[rows].astype(F32)).astype(BF16)
            return carry

        lax.fori_loop(0, 8, add_rows, 0)
        copy = pltpu.make_async_copy(sum_ref, out_ref.at[pl.ds(0, count)], sem)
        copy.start()
    else:
        m_ref, own_ref, send_ref = refs
    project(p_ref, m_ref, wo_ref, wb0_ref, wb1_ref, own_ref, send_ref)
    if done:
        copy.wait()


def mix(weights, start, count, w_out, other, mids=None, after=None, m=None, done=None, total=0):
    cols = weights.shape[1]
    rows = w_out.shape[0]
    width = other.shape[1]
    skip = (other.shape[0] - 2 * rows) // rows
    tile = count if done else min(1024, count)
    base = start // tile
    args = [weights, w_out, other, other]
    in_specs = [pl.BlockSpec((tile, cols), lambda i: (base + i, 0)), whole(w_out.shape)]
    in_specs += [pl.BlockSpec((rows, width), functools.partial(lambda j, i: (j, 0), skip + j)) for j in range(2)]
    out_specs = [pl.BlockSpec((tile, width), lambda i: (i, 0))] * 2
    out_shape = [jax.ShapeDtypeStruct((count, width), BF16)] * 2
    scratch = []
    if m is None:
        args += [*mids, after]
        in_specs += [whole(x.shape) for x in mids] + [pl.BlockSpec(memory_space=pl.ANY)]
        out_specs += [whole((cols, LANDMARKS))]
        out_shape += [jax.ShapeDtypeStruct((cols, LANDMARKS), BF16)]
    else:
        args += [m]
        in_specs += [whole(m.shape)]
    if done:
        args += list(done)
        in_specs += [whole(x.shape) for x in done]
        out_specs += [pl.BlockSpec(memory_space=pl.ANY)]
        scratch = [pltpu.VMEM(done[0].shape, BF16), pltpu.SemaphoreType.DMA]
        out_shape += [jax.ShapeDtypeStruct((total, width), BF16)]
    return pl.pallas_call(
        functools.partial(mix_kernel, m is None, 1 if done else 0),
        grid=(count // tile,),
        in_specs=in_specs,
        out_specs=out_specs,
        out_shape=out_shape,
        scratch_shapes=scratch,
        compiler_params=params(16),
        cost_estimate=cost(2 * count * (cols * 256 + 4 * rows * width), count * 4096),
        name="mix",
    )(*args)


def add_kernel(own_ref, got_ref, *refs):
    refs[-1][...] = (own_ref[...].astype(F32) + got_ref[...].astype(F32)).astype(BF16)


def add_into(out, own, got, start, total):
    count, width = own.shape
    tile = min(1024, count)
    base = start // tile
    row = pl.BlockSpec((tile, width), lambda i: (i, 0))
    old = [] if out is None else [out]
    return pl.pallas_call(
        add_kernel,
        grid=(count // tile,),
        in_specs=[row, row] + [pl.BlockSpec(memory_space=pl.ANY)] * len(old),
        out_specs=pl.BlockSpec((tile, width), lambda i: (base + i, 0)),
        out_shape=jax.ShapeDtypeStruct((total, width), BF16),
        input_output_aliases={2: 0} if old else {},
        compiler_params=params(4),
        cost_estimate=cost(500_000_000, 6 * own.size),
        name="add",
    )(own, got, *old)


def swap(x, axes, sizes, steps):
    pairs = []
    total = math.prod(sizes)
    for i in range(total):
        rest, at = i, []
        for size in reversed(sizes):
            at.append(rest % size)
            rest //= size
        at = [a ^ s for a, s in zip(reversed(at), steps)]
        to = 0
        for a, size in zip(at, sizes):
            to = to * size + a
        pairs.append((i, to))
    return lax.ppermute(x, axes if len(axes) > 1 else axes[0], pairs)


def gather_doubling(x, n_seq):
    bit = n_seq // 2
    while bit:
        y = swap(x, ("seq",), (n_seq,), (bit,))
        x, *keys = in_order(x, y, bit, bit == 1)
        bit //= 2
    return x, keys[0]


def on_device(n_seq, n_tp, tokens, w_qkv, w_out):
    width = w_out.shape[0]
    heads = width // HEAD_DIM
    far = n_tp // 2

    means, tokens = token_means(tokens, LANDMARKS // n_seq)
    local = local_marks(means, w_qkv)
    send, w_value_t = prepare(w_qkv, w_out, far)
    other = swap(send, ("tp",), (n_tp,), (far,))
    marks, k_marks = gather_doubling(local, n_seq)
    keys = project_rows(tokens, w_qkv, 1)
    queries = project_rows(tokens, w_qkv, 0)
    values_t = project_values(tokens, w_value_t)
    k_other = swap(k_marks, ("tp",), (n_tp,), (far,))

    mine, theirs = block_partials(keys, values_t, marks, heads)
    pair = merge_pair(mine, swap(theirs, ("seq",), (n_seq,), (1,)))
    parts = [pair] + [swap(pair, ("seq",), (n_seq,), (2 * j,)) for j in reversed(range(1, n_seq // 2))]
    pinv, early = pseudo_inverse(marks, heads, k_other, tokens, queries, other)
    mid = middle_rows(parts, pinv)
    sizes = (n_seq, n_tp)
    mids = [mid] + [swap(mid, ("seq", "tp"), sizes, s) for s in ((1, 0), (0, far), (1, far))]
    total, done = tokens.shape[0], early.shape[0]
    half = total // 2
    late = late_weights(done, heads, tokens, queries, other, marks, k_other)

    def cross(x):
        return swap(x, ("tp",), (n_tp,), (1,))

    own0, send0, m = mix(early, 0, half, w_out, other, mids=mids, after=late)
    got0 = cross(send0)
    own1, send1 = mix(early, half, done - half, w_out, other, m=m)
    got1 = cross(send1)
    own2, send2, out = mix(late, 0, total - done, w_out, other, m=m, done=(own0, got0), total=total)
    out = add_into(out, own1, got1, half, total)
    return add_into(out, own2, cross(send2), done, total)


def solution(mesh):
    n_seq, n_tp = mesh.shape["seq"], mesh.shape["tp"]
    if n_tp != 4 or n_seq < 2 or n_seq & (n_seq - 1):
        raise ValueError("unsupported mesh")
    in_specs = (P("seq", None), P(None, None, "tp"), P("tp", None))
    return jax.shard_map(
        functools.partial(on_device, n_seq, n_tp),
        mesh=mesh,
        in_specs=in_specs,
        out_specs=P("seq", "tp"),
        check_vma=False,
    )
```
